32 devices in a mesh: ctx: 4 (over y, x), fsdp: 8 (over z, core).
Axes of the slice: x: 2, y: 2, z: 4, core: 2. Of those that a mesh axis runs over, the one named last changes fastest.
Arguments:
- hidden_in: bfloat16 [8, 512, 2048], P('fsdp', 'ctx'), may hold values from -6 to 6
- block_order: int32 [8, 8], P('fsdp'), may hold values from 0 to 7, each once within a row
- w_query: bfloat16 [2048, 2048], P('fsdp'), may hold values from -0.125 to 0.125
- w_key: bfloat16 [2048, 2048], P('fsdp'), may hold values from -0.125 to 0.125
- w_value: bfloat16 [2048, 2048], P('fsdp'), may hold values from -0.125 to 0.125
- w_output: bfloat16 [2048, 2048], P('fsdp'), may hold values from -0.125 to 0.125
- w_gate: bfloat16 [2048, 8192], P(None, 'fsdp'), may hold values from -0.125 to 0.125
- w_up: bfloat16 [2048, 8192], P(None, 'fsdp'), may hold values from -0.125 to 0.125
- w_down: bfloat16 [8192, 2048], P('fsdp'), may hold values from -0.0625 to 0.0625
- norm_gains: bfloat16 [4, 2048], P(None, 'fsdp'), may hold values from 0.3 to 5.5
- out_grad: bfloat16 [8, 512, 2048], P('fsdp', 'ctx'), may hold values from -6 to 6
Outputs:
- block_out: bfloat16 [8, 512, 2048], P('fsdp', 'ctx')
- input_grad: float32 [8, 512, 2048], P('fsdp', 'ctx')
- grad_query: float32 [2048, 2048], P('fsdp')
- grad_key: float32 [2048, 2048], P('fsdp')
- grad_value: float32 [2048, 2048], P('fsdp')
- grad_output: float32 [2048, 2048], P('fsdp')
- grad_gate: float32 [2048, 8192], P(None, 'fsdp')
- grad_up: float32 [2048, 8192], P(None, 'fsdp')
- grad_down: float32 [8192, 2048], P('fsdp')
- grad_gains: float32 [4, 2048], P(None, 'fsdp')
The draws below stay inside these ranges and needn't reach their ends.
Inputs may be any that keep to these rules, and one draw needn't show every extreme that they name: `block_order`: each row names every block 0 to 7 once; entry j is the block of that sequence held in rows j * 64 to (j + 1) * 64 - 1.
All inputs are finite; a program needn't handle non-finite values.
Results may differ from the reference program's by a relative error of at most 0.023.
The reference program's roundings to bfloat16 on the way count: a program that leaves them out, or rounds other values in their place, can miss the bound.
Values may be sent and summed in bfloat16 or wider, within the bound.
A program may use at most 320 MiB of HBM per device.

```python
import jax
import jax.numpy as jnp
from jax import lax

D = 2048
HEADS = 16
HEAD_DIM = 128
FF = 8192
BLK = 64
BLOCKS = 8
SEQ_LEN = 512
SEQS = 8


def draw_norm_gains(key, part):
    first, second = jax.random.split(jax.random.fold_in(key, 17))
    qk_rows = jax.random.uniform(first, (2, D), jnp.float32, 0.5, 2.0)
    post_rows = jax.random.uniform(second, (2, D), jnp.float32, 0.5, 1.5)
    return jnp.concatenate([qk_rows, post_rows], axis=0).astype(jnp.bfloat16)


def levels(key, dims, pieces, low, top_value):
    level = 1.0
    for axis_at, parts in pieces:
        draws = jax.random.uniform(jax.random.fold_in(jax.random.fold_in(key, 6), axis_at), (parts,), jnp.float32, low / len(pieces), top_value / len(pieces))
        level = level * jnp.repeat(jnp.exp(draws), dims[axis_at] // parts).reshape((-1,) + (1,) * (len(dims) - 1 - axis_at))
    return level


def scatter_about(own_key, dims, deviation, most, cuts=(), kind=jnp.bfloat16):
    drawn = deviation * jax.random.normal(own_key, dims, jnp.float32)
    if cuts:
        drawn = drawn * levels(own_key, dims, cuts, -0.22, 0.18)
    return jnp.clip(drawn, -most, most).astype(kind)


def setup_inputs(seed: int = 0) -> dict:
    key_list = jax.random.split(jax.random.key(seed), 12)
    return {
        "hidden_in": scatter_about(key_list[0], (SEQS, SEQ_LEN, D), 1.0, 6.0, ((0, 8), (1, 4))),
        "block_order": jax.vmap(lambda own: jax.random.permutation(own, BLOCKS))(jax.random.split(key_list[1], SEQS)).reshape((SEQS, BLOCKS)).astype(jnp.int32),
        "w_query": scatter_about(key_list[2], (D, D), D ** -0.5, 0.125, ((0, 8),)),
        "w_key": scatter_about(key_list[3], (D, D), D ** -0.5, 0.125, ((0, 8),)),
        "w_value": scatter_about(key_list[4], (D, D), D ** -0.5, 0.125, ((0, 8),)),
        "w_output": scatter_about(key_list[5], (D, D), D ** -0.5, 0.125, ((0, 8),)),
        "w_gate": scatter_about(key_list[6], (D, FF), D ** -0.5, 0.125, ((1, 8),)),
        "w_up": scatter_about(key_list[7], (D, FF), D ** -0.5, 0.125, ((1, 8),)),
        "w_down": scatter_about(key_list[8], (FF, D), FF ** -0.5, 0.0625, ((0, 8),)),
        "norm_gains": draw_norm_gains(jax.random.fold_in(key_list[11], 71), 0),
        "out_grad": scatter_about(key_list[10], (SEQS, SEQ_LEN, D), 1.0, 6.0, ((0, 8), (1, 4))),
    }


norm_eps = 1e-06
rope_base = 500000.0
neg_fill = -1e+30

@jax.custom_vjp
def low(v):
    return lax.optimization_barrier(v.astype(jnp.bfloat16)).astype(jnp.float32)

@jax.custom_vjp
def low_back(v):
    return v

def low_keep(v):
    return (low(v), None)

def low_pass(kept, grad):
    return (grad,)

def back_keep(v):
    return (v, None)

def back_low(kept, grad):
    return (low(grad),)
low.defvjp(low_keep, low_pass)
low_back.defvjp(back_keep, back_low)

def matmul(left, right):
    return jnp.dot(left, right, precision=lax.Precision.HIGHEST)

def rms_norm(values, gain):
    return values * lax.rsqrt(lax.optimization_barrier(jnp.mean(values * values, axis=-1, keepdims=True)) + norm_eps) * gain

def rotate_half(values):
    half_width = values.shape[-1] // 2
    return jnp.concatenate([-values[..., half_width:], values[..., :half_width]], axis=-1)

def rope_tables(positions, width):
    half_width = width // 2
    inverse = rope_base ** (-(jnp.arange(half_width, dtype=jnp.float32) * 2.0) / width)
    angle = positions.astype(jnp.float32)[:, None] * inverse[None, :]
    cosine = jnp.concatenate([jnp.cos(angle), jnp.cos(angle)], axis=-1)
    sine = jnp.concatenate([jnp.sin(angle), jnp.sin(angle)], axis=-1)
    return (cosine[:, None, :], sine[:, None, :])

def apply_rope(values, cosine, sine):
    shaped = values.reshape(values.shape[0], HEADS, HEAD_DIM)
    return shaped * cosine + rotate_half(shaped) * sine

def one_sequence(params, pair):
    tokens, positions = pair
    w_query, w_key, w_value, w_output, w_gate, w_up, w_down, gains = params
    score_scale = HEAD_DIM ** (-0.5)
    cosine, sine = rope_tables(positions, HEAD_DIM)
    query_raw = low_back(matmul(tokens, w_query))
    key_raw = low_back(matmul(tokens, w_key))
    queries = low(apply_rope(rms_norm(query_raw, gains[0]), cosine, sine))
    keys = low(apply_rope(rms_norm(key_raw, gains[1]), cosine, sine))
    values = low_back(low(matmul(tokens, w_value))).reshape(tokens.shape[0], HEADS, HEAD_DIM)
    scores = jnp.einsum('qhd,khd->hqk', queries, keys, precision=lax.Precision.HIGHEST) * score_scale
    allowed = positions[None, :] <= positions[:, None]
    scores = low_back(jnp.where(allowed[None], scores, neg_fill))
    shifted = scores - lax.optimization_barrier(jnp.max(scores, axis=-1, keepdims=True))
    expd = jnp.exp(shifted)
    probs = expd / lax.optimization_barrier(jnp.sum(expd, axis=-1, keepdims=True))
    mixed = jnp.einsum('hqk,khd->qhd', low(probs), values, precision=lax.Precision.HIGHEST)
    mixed = low_back(low(mixed.reshape(tokens.shape[0], HEADS * HEAD_DIM)))
    projected = low_back(matmul(mixed, w_output))
    residual = tokens + rms_norm(projected, gains[2])
    normed_in = low(residual)
    gate = low_back(matmul(normed_in, w_gate))
    upward = low_back(matmul(normed_in, w_up))
    hidden = low(gate * jax.nn.sigmoid(gate) * upward)
    mlp_out = low_back(matmul(hidden, w_down))
    return residual + rms_norm(mlp_out, gains[3])

def forward(tokens, w_query, w_key, w_value, w_output, w_gate, w_up, w_down, gains, positions):
    params = (w_query, w_key, w_value, w_output, w_gate, w_up, w_down, gains)
    layer = jax.checkpoint(lambda pair: one_sequence(params, pair))
    return lax.map(layer, (tokens, positions))

def reference(hidden_in, block_order, w_query, w_key, w_value, w_output, w_gate, w_up, w_down, norm_gains, out_grad):
    offsets = jnp.arange(BLK, dtype=jnp.int32)
    positions = (block_order[:, :, None] * BLK + offsets[None, None, :]).reshape(SEQS, SEQ_LEN).astype(jnp.int32)
    floats = [item.astype(jnp.float32) for item in (hidden_in, w_query, w_key, w_value, w_output, w_gate, w_up, w_down, norm_gains)]
    result, pullback = jax.vjp(lambda *items: forward(*items, positions), *floats)
    grads = pullback(out_grad.astype(jnp.float32))
    return (result.astype(jnp.bfloat16), grads[0], grads[1], grads[2], grads[3], grads[4], grads[5], grads[6], grads[7], grads[8])
```

```python
import functools

import jax
import jax.numpy as jnp
from jax import lax
from jax.experimental import pallas as pl
from jax.experimental.pallas import tpu as pltpu
from jax.sharding import PartitionSpec as P

HEADS = 16
HEAD_DIM = 128

norm_eps = 1e-06
rope_base = 500000.0
neg_fill = -1e30

MESH = pl.DeviceIdType.MESH
f32 = jnp.float32
bf16 = jnp.bfloat16


def anywhere():
    return pl.BlockSpec(memory_space=pl.ANY)


def in_vmem():
    return pl.BlockSpec(memory_space=pltpu.VMEM)


def remote(source, target, sent, landed, where):
    return pltpu.make_async_remote_copy(
        src_ref=source,
        dst_ref=target,
        send_sem=sent,
        recv_sem=landed,
        device_id=where,
        device_id_type=MESH,
    )


def exchange_kernel(axis, size, scatter, count, *refs):
    given, kept = refs[:count], refs[count : 2 * count]
    own_sem, send_sem, land_sem = refs[2 * count :]
    own = lax.axis_index(axis)
    barrier = pltpu.get_barrier_semaphore()
    for step in range(1, size):
        pl.semaphore_signal(
            barrier, inc=1, device_id={axis: lax.rem(own + step, size)}, device_id_type=MESH
        )
    local = []
    for item in range(count):
        source = given[item].at[own] if scatter else given[item]
        local.append(pltpu.make_async_copy(source, kept[item].at[own], own_sem.at[item]))
        local[-1].start()
    pl.semaphore_wait(barrier, size - 1)
    copies = []
    for step in range(1, size):
        peer = lax.rem(own + step, size)
        for item in range(count):
            source = given[item].at[peer] if scatter else given[item]
            copies.append(
                remote(
                    source,
                    kept[item].at[own],
                    send_sem.at[item, step],
                    land_sem.at[item, step],
                    {axis: peer},
                )
            )
            copies[-1].start()
    for copy in local:
        copy.wait()
    for copy in copies:
        copy.wait()


def exchange(axis, arrays, key, scatter=True):
    size = lax.axis_size(axis)
    count = len(arrays)
    shapes = [
        jax.ShapeDtypeStruct(item.shape if scatter else (size,) + item.shape, item.dtype)
        for item in arrays
    ]
    return pl.pallas_call(
        functools.partial(exchange_kernel, axis, size, scatter, count),
        out_shape=shapes,
        in_specs=[in_vmem()] * count,
        out_specs=[anywhere()] * count,
        scratch_shapes=[
            pltpu.SemaphoreType.DMA((count,)),
            pltpu.SemaphoreType.DMA((count, size)),
            pltpu.SemaphoreType.DMA((count, size)),
        ],
        compiler_params=pltpu.CompilerParams(collective_id=key, has_side_effects=True),
        name=f"exchange_{axis}_{key}",
    )(*arrays)


def greet_line(own, chips):
    chip, core = own // 2, own % 2
    barrier = pltpu.get_barrier_semaphore()

    def greet(place):
        pl.semaphore_signal(barrier, inc=1, device_id={"fsdp": place}, device_id_type=MESH)

    greet(chip * 2 + 1 - core)

    @pl.when(chip > 0)
    def _():
        greet(own - 2)

    @pl.when(chip < chips - 1)
    def _():
        greet(own + 2)

    expected = 1 + jnp.minimum(chip, 1) + jnp.minimum(chips - 1 - chip, 1)
    pl.semaphore_wait(barrier, expected)


def gather_kernel(chips, given, kept, own_sem, send_sem, land_sem):
    own = lax.axis_index("fsdp")
    chip, core = own // 2, own % 2
    sibling = chip * 2 + 1 - core
    local = pltpu.make_async_copy(given, kept.at[own], own_sem)
    local.start()
    greet_line(own, chips)

    def copy(source, place, way, step, target):
        return remote(
            source, kept.at[place], send_sem.at[way, step], land_sem.at[place], {"fsdp": target}
        )

    @pl.when(chip < chips - 1)
    def _():
        copy(given, own, 0, 0, own + 2).start()

    @pl.when(chip > 0)
    def _():
        copy(given, own, 1, 0, own - 2).start()

    copy(given, own, 2, 0, sibling).start()
    local.wait()
    for step in range(1, chips):
        from_left, from_right = own - 2 * step, own + 2 * step

        @pl.when(chip >= step)
        def _():
            copy(kept.at[from_left], from_left, 0, step, own).wait_recv()

            @pl.when(chip < chips - 1)
            def _():
                copy(kept.at[from_left], from_left, 0, step, own + 2).start()

            copy(kept.at[from_left], from_left, 2, step, sibling).start()

        @pl.when(chip + step < chips)
        def _():
            copy(kept.at[from_right], from_right, 1, step, own).wait_recv()

            @pl.when(chip > 0)
            def _():
                copy(kept.at[from_right], from_right, 1, step, own - 2).start()

            copy(kept.at[from_right], from_right, 3, step, sibling).start()

    for other in range(chips):
        place = other * 2 + 1 - core
        copy(kept.at[place], place, 2, 0, sibling).wait_recv()

    @pl.when(chip < chips - 1)
    def _():
        copy(given, own, 0, 0, own + 2).wait_send()

    @pl.when(chip > 0)
    def _():
        copy(given, own, 1, 0, own - 2).wait_send()

    copy(given, own, 2, 0, sibling).wait_send()
    for step in range(1, chips):
        from_left, from_right = own - 2 * step, own + 2 * step

        @pl.when(chip >= step)
        def _():
            @pl.when(chip < chips - 1)
            def _():
                copy(kept.at[from_left], from_left, 0, step, own + 2).wait_send()

            copy(kept.at[from_left], from_left, 2, step, sibling).wait_send()

        @pl.when(chip + step < chips)
        def _():
            @pl.when(chip > 0)
            def _():
                copy(kept.at[from_right], from_right, 1, step, own - 2).wait_send()

            copy(kept.at[from_right], from_right, 3, step, sibling).wait_send()


def gather_line(shard, key):
    size = lax.axis_size("fsdp")
    chips = size // 2
    kept = pl.pallas_call(
        functools.partial(gather_kernel, chips),
        out_shape=jax.ShapeDtypeStruct((size,) + shard.shape, shard.dtype),
        in_specs=[in_vmem()],
        out_specs=anywhere(),
        scratch_shapes=[
            pltpu.SemaphoreType.DMA,
            pltpu.SemaphoreType.DMA((4, chips)),
            pltpu.SemaphoreType.DMA((size,)),
        ],
        compiler_params=pltpu.CompilerParams(collective_id=key, has_side_effects=True),
        name=f"gather_line_{key}",
    )(shard)
    return kept.reshape((size * shard.shape[0],) + shard.shape[1:])


def reduce_kernel(
    chips,
    wire,
    given,
    total,
    mine,
    beside,
    from_left,
    from_right,
    outgoing,
    load_sem,
    side_send,
    side_land,
    line_send,
    left_land,
    right_land,
):
    own = lax.axis_index("fsdp")
    chip, core = own // 2, own % 2
    sibling = chip * 2 + 1 - core

    def load(other):
        return pltpu.make_async_copy(given.at[other * 2 + core], mine.at[other], load_sem.at[other])

    def side(other):
        return remote(
            given.at[other * 2 + 1 - core],
            beside.at[other],
            side_send.at[other],
            side_land.at[other],
            {"fsdp": sibling},
        )

    def rightward(other, target):
        return remote(
            outgoing.at[other],
            from_left.at[other],
            line_send.at[other],
            left_land.at[other],
            {"fsdp": target},
        )

    def leftward(other, target):
        return remote(
            outgoing.at[other],
            from_right.at[other],
            line_send.at[other],
            right_land.at[other],
            {"fsdp": target},
        )

    for other in range(chips):
        load(other).start()
    greet_line(own, chips)
    for tick in range(chips - 1):
        right_to = chips - 1 - (tick - chip)
        left_to = tick - (chips - 1 - chip)

        @pl.when((tick >= chip) & (right_to > chip))
        def _():
            side(right_to).start()

        @pl.when((left_to >= 0) & (left_to < chip))
        def _():
            side(left_to).start()

    side(chip).start()
    for tick in range(chips - 1):
        right_to = chips - 1 - (tick - chip)
        left_to = tick - (chips - 1 - chip)

        @pl.when((tick >= chip) & (right_to > chip))
        def _():
            load(right_to).wait()
            side(right_to).wait_recv()

            @pl.when(chip > 0)
            def _():
                rightward(right_to, own).wait_recv()
                outgoing[right_to] = (
                    mine[right_to] + beside[right_to] + from_left[right_to].astype(f32)
                ).astype(wire)

            @pl.when(chip == 0)
            def _():
                outgoing[right_to] = (mine[right_to] + beside[right_to]).astype(wire)

            rightward(right_to, own + 2).start()

        @pl.when((left_to >= 0) & (left_to < chip))
        def _():
            load(left_to).wait()
            side(left_to).wait_recv()

            @pl.when(chip < chips - 1)
            def _():
                leftward(left_to, own).wait_recv()
                outgoing[left_to] = (
                    mine[left_to] + beside[left_to] + from_right[left_to].astype(f32)
                ).astype(wire)

            @pl.when(chip == chips - 1)
            def _():
                outgoing[left_to] = (mine[left_to] + beside[left_to]).astype(wire)

            leftward(left_to, own - 2).start()

    load(chip).wait()
    side(chip).wait_recv()
    total[...] = mine[chip] + beside[chip]

    @pl.when(chip > 0)
    def _():
        rightward(chip, own).wait_recv()
        total[...] += from_left[chip].astype(f32)

    @pl.when(chip < chips - 1)
    def _():
        leftward(chip, own).wait_recv()
        total[...] += from_right[chip].astype(f32)

    for other in range(chips):
        side(other).wait_send()

        @pl.when(chip != other)
        def _():
            rightward(other, own).wait_send()


def reduce_line(partial, key, wire=f32):
    size, rows, width = partial.shape
    chips = size // 2
    return pl.pallas_call(
        functools.partial(reduce_kernel, chips, wire),
        out_shape=jax.ShapeDtypeStruct((rows, width), f32),
        in_specs=[anywhere()],
        out_specs=in_vmem(),
        scratch_shapes=[
            pltpu.VMEM((chips, rows, width), f32),
            pltpu.VMEM((chips, rows, width), f32),
            pltpu.VMEM((chips, rows, width), wire),
            pltpu.VMEM((chips, rows, width), wire),
            pltpu.VMEM((chips, rows, width), wire),
            pltpu.SemaphoreType.DMA((chips,)),
            pltpu.SemaphoreType.DMA((chips,)),
            pltpu.SemaphoreType.DMA((chips,)),
            pltpu.SemaphoreType.DMA((chips,)),
            pltpu.SemaphoreType.DMA((chips,)),
            pltpu.SemaphoreType.DMA((chips,)),
        ],
        compiler_params=pltpu.CompilerParams(
            collective_id=key, has_side_effects=True, vmem_limit_bytes=60 * 1024 * 1024
        ),
        name=f"reduce_line_{key}",
    )(partial)


def probs_of(query, key, query_pos, key_pos):
    scores = lax.dot_general(
        query, key, (((1,), (1,)), ((), ())), preferred_element_type=f32
    ) * (HEAD_DIM ** (-0.5))
    scores = jnp.where(key_pos <= query_pos, scores, neg_fill)
    expd = jnp.exp(scores - jnp.max(scores, axis=-1, keepdims=True))
    return expd / jnp.sum(expd, axis=-1, keepdims=True)


def flat(ref):
    return ref[...].reshape(ref.shape[0] * ref.shape[-2], ref.shape[-1])


def attend_kernel(query_ref, key_ref, value_ref, query_pos, key_pos, mixed_ref):
    probs = probs_of(flat(query_ref), flat(key_ref), query_pos[...], key_pos[...])
    mixed_ref[...] = jnp.dot(
        probs.astype(bf16), flat(value_ref), preferred_element_type=f32
    ).astype(bf16)


def attend_back_kernel(
    query_ref,
    key_ref,
    value_ref,
    query_pos,
    key_pos,
    grad_ref,
    grad_query_ref,
    grad_key_ref,
    grad_value_ref,
    key_sum,
    value_sum,
):
    step, steps = pl.program_id(2), pl.num_programs(2)
    score_scale = HEAD_DIM ** (-0.5)
    query, key, value = flat(query_ref), flat(key_ref), flat(value_ref)
    grad = grad_ref[...]
    probs = probs_of(query, key, query_pos[...], key_pos[...])
    grad_probs = lax.dot_general(
        grad, value, (((1,), (1,)), ((), ())), preferred_element_type=f32
    )
    grad_scores = (
        probs * (grad_probs - jnp.sum(probs * grad_probs, axis=-1, keepdims=True))
    ).astype(bf16)
    grad_query_ref[...] = jnp.dot(grad_scores, key, preferred_element_type=f32) * score_scale
    value_part = lax.dot_general(
        probs.astype(bf16), grad, (((0,), (0,)), ((), ())), preferred_element_type=f32
    )
    key_part = lax.dot_general(
        grad_scores, query, (((0,), (0,)), ((), ())), preferred_element_type=f32
    )

    @pl.when(step == 0)
    def _():
        key_sum[...] = key_part
        value_sum[...] = value_part

    @pl.when(step > 0)
    def _():
        key_sum[...] += key_part
        value_sum[...] += value_part

    @pl.when(step == steps - 1)
    def _():
        grad_key_ref[...] = (key_sum[...] * score_scale).reshape(grad_key_ref.shape)
        grad_value_ref[...] = value_sum[...].astype(bf16).reshape(grad_value_ref.shape)


def attention_specs(parts, rows, seq_rows):
    query = pl.BlockSpec((1, None, None, rows, HEAD_DIM), lambda i, h, c: (c, 0, i, 0, h))
    key = pl.BlockSpec((parts, None, None, rows, HEAD_DIM), lambda i, h, c: (0, 1, i, 0, h))
    value = pl.BlockSpec((parts, None, None, rows, HEAD_DIM), lambda i, h, c: (0, 2, i, 0, h))
    query_pos = pl.BlockSpec((None, None, rows, 1), lambda i, h, c: (i, c, 0, 0))
    key_pos = pl.BlockSpec((None, 1, seq_rows), lambda i, h, c: (i, 0, 0))
    row_block = pl.BlockSpec((None, None, rows, HEAD_DIM), lambda i, h, c: (c, i, 0, h))
    all_block = pl.BlockSpec((parts, None, rows, HEAD_DIM), lambda i, h, c: (0, i, 0, h))
    return [query, key, value, query_pos, key_pos], row_block, all_block


def attend(packed, query_pos, key_pos):
    parts, _, pair, rows, width = packed.shape
    seq_rows = parts * rows
    in_specs, row_block, _ = attention_specs(parts, rows, seq_rows)
    return pl.pallas_call(
        attend_kernel,
        grid=(pair, width // HEAD_DIM, parts),
        out_shape=jax.ShapeDtypeStruct((parts, pair, rows, width), bf16),
        in_specs=in_specs,
        out_specs=row_block,
        name="attend",
    )(packed, packed, packed, query_pos, key_pos)


def attend_back(packed, query_pos, key_pos, grad):
    parts, _, pair, rows, width = packed.shape
    seq_rows = parts * rows
    in_specs, row_block, all_block = attention_specs(parts, rows, seq_rows)
    return pl.pallas_call(
        attend_back_kernel,
        grid=(pair, width // HEAD_DIM, parts),
        out_shape=[
            jax.ShapeDtypeStruct((parts, pair, rows, width), f32),
            jax.ShapeDtypeStruct((parts, pair, rows, width), f32),
            jax.ShapeDtypeStruct((parts, pair, rows, width), bf16),
        ],
        in_specs=in_specs + [row_block],
        out_specs=[row_block, all_block, all_block],
        scratch_shapes=[
            pltpu.VMEM((seq_rows, HEAD_DIM), f32),
            pltpu.VMEM((seq_rows, HEAD_DIM), f32),
        ],
        name="attend_back",
    )(packed, packed, packed, query_pos, key_pos, grad)


def norm_stat(values):
    return lax.rsqrt(jnp.mean(values * values, axis=-1, keepdims=True) + norm_eps)


def norm_back(values, scale, gain, grad_out):
    weighted = grad_out * gain
    grad_values = scale * weighted - values * (scale * scale * scale) * jnp.mean(
        weighted * values, axis=-1, keepdims=True
    )
    grad_gain = jnp.sum(grad_out * (values * scale), axis=0)
    return (grad_values, grad_gain)


def rotate_half(values):
    half_width = values.shape[-1] // 2
    return jnp.concatenate([-values[..., half_width:], values[..., :half_width]], axis=-1)


def rope_tables(positions, width):
    half_width = width // 2
    inverse = rope_base ** (-(jnp.arange(half_width, dtype=f32) * 2.0) / width)
    angle = positions.astype(f32)[:, None] * inverse[None, :]
    cosine = jnp.concatenate([jnp.cos(angle), jnp.cos(angle)], axis=-1)
    sine = jnp.concatenate([jnp.sin(angle), jnp.sin(angle)], axis=-1)
    return (cosine[:, None, :], sine[:, None, :])


def by_head(values):
    return values.reshape(values.shape[0], values.shape[1] // HEAD_DIM, HEAD_DIM)


def apply_rope(values, cosine, sine):
    shaped = by_head(values)
    return (shaped * cosine + rotate_half(shaped) * sine).reshape(values.shape)


def rope_back(grads, cosine, sine):
    shaped = by_head(grads)
    return (shaped * cosine - rotate_half(shaped * sine)).reshape(grads.shape)


def mm(left, right):
    return jnp.dot(left, right, preferred_element_type=f32)


def mm_nt(left, right):
    return lax.dot_general(left, right, (((1,), (1,)), ((), ())), preferred_element_type=f32)


def mm_tn(left, right):
    return lax.dot_general(left, right, (((0,), (0,)), ((), ())), preferred_element_type=f32)


def shards(
    hidden_in,
    block_order,
    w_query,
    w_key,
    w_value,
    w_output,
    w_gate,
    w_up,
    w_down,
    norm_gains,
    out_grad,
):
    rows, width = hidden_in.shape[1:]
    parts, owners = lax.axis_size("ctx"), lax.axis_size("fsdp")
    part, owner = lax.axis_index("ctx"), lax.axis_index("fsdp")
    group = owners * rows
    own_width = width // owners
    pair = owners // parts
    blocks = block_order.shape[1]
    block_rows = parts * rows // blocks
    piece = w_query.shape[0] // parts
    tokens_b = hidden_in[0]
    tokens_f = tokens_b.astype(f32)

    small = jnp.concatenate(
        [
            norm_gains.astype(f32),
            jnp.pad(block_order.astype(f32), ((0, 0), (0, own_width - blocks))),
        ],
        axis=0,
    )
    (small_all,) = exchange("fsdp", [small], 0, scatter=False)
    gains = small_all[:, :4].transpose(1, 0, 2).reshape(4, width)
    orders = small_all[:, 4, :blocks].astype(jnp.int32)
    own_gains = norm_gains.astype(f32)
    stacked = jnp.stack(
        [
            lax.dynamic_slice_in_dim(item, part * piece, piece)
            for item in (w_query, w_key, w_value)
        ]
    )
    stacked = stacked.reshape(3, piece, owners, own_width).transpose(2, 1, 0, 3)
    (columns,) = exchange("fsdp", [stacked.reshape(owners, piece, 3 * own_width)], 1)
    (columns,) = exchange("ctx", [columns], 2, scatter=False)
    w_heads = columns.transpose(1, 0, 2, 3).reshape(width, 3 * own_width)
    group_tokens = gather_line(tokens_b, 3)
    full_output = lax.all_gather(w_output, "fsdp", axis=0, tiled=True)

    offsets = jnp.arange(block_rows, dtype=jnp.int32)
    seq_pos = (orders[:, :, None] * block_rows + offsets[None, None, :]).reshape(
        owners, parts * rows
    )
    group_pos = lax.dynamic_slice_in_dim(seq_pos, part * rows, rows, 1).reshape(group)
    pair_pos = lax.dynamic_slice_in_dim(seq_pos, part * pair, pair, 0)
    query_pos = pair_pos.reshape(pair, parts, rows, 1)
    key_pos = pair_pos.reshape(pair, 1, parts * rows)
    cosine, sine = rope_tables(group_pos, HEAD_DIM)

    raw = mm(group_tokens, w_heads)
    query_raw, key_raw = raw[:, :own_width], raw[:, own_width : 2 * own_width]
    values = raw[:, 2 * own_width :].astype(bf16)
    squares = jnp.stack(
        [jnp.sum(query_raw * query_raw, axis=-1), jnp.sum(key_raw * key_raw, axis=-1)]
    )
    (squares,) = exchange("fsdp", [squares], 4, scatter=False)
    scales = lax.rsqrt(jnp.sum(squares, axis=0) / width + norm_eps)
    query_scale, key_scale = scales[0][:, None], scales[1][:, None]
    queries = apply_rope(query_raw * query_scale * own_gains[0], cosine, sine).astype(bf16)
    keys = apply_rope(key_raw * key_scale * own_gains[1], cosine, sine).astype(bf16)
    packed = jnp.stack(
        [item.reshape(parts, pair, rows, own_width) for item in (queries, keys, values)], axis=1
    )
    (packed,) = exchange("ctx", [packed], 5)
    mixed_pair = attend(packed, query_pos, key_pos)
    (mixed_group,) = exchange("ctx", [mixed_pair], 6)
    mixed_group = mixed_group.reshape(owners, rows, own_width)
    (mixed_own,) = exchange("fsdp", [mixed_group], 7)
    mixed_own = mixed_own.transpose(1, 0, 2).reshape(rows, width)
    projected = mm(mixed_own, full_output)
    proj_scale = norm_stat(projected)
    residual = tokens_f + projected * proj_scale * gains[2]
    mlp_rows_in = gather_line(residual.astype(bf16), 8)
    gate = mm(mlp_rows_in, w_gate)
    upward = mm(mlp_rows_in, w_up)
    sigma = jax.nn.sigmoid(gate)
    hidden_b = (gate * sigma * upward).astype(bf16)
    mlp_out = reduce_line(mm(hidden_b, w_down).reshape(owners, rows, width), 9)
    mlp_scale = norm_stat(mlp_out)
    block_out = residual + mlp_out * mlp_scale * gains[3]

    grad_y = out_grad[0].astype(f32)
    grad_mlp, gain_ff = norm_back(mlp_out, mlp_scale, gains[3], grad_y)
    grad_rows = gather_line(grad_mlp.astype(bf16), 10)
    grad_hidden = mm_nt(grad_rows, w_down)
    grad_gate_b = (grad_hidden * upward * sigma * (1.0 + gate * (1.0 - sigma))).astype(bf16)
    grad_up_b = (grad_hidden * (gate * sigma)).astype(bf16)
    down_sum = lax.psum(mm_tn(hidden_b, grad_rows).astype(bf16), "ctx").astype(f32)
    gate_sum = lax.psum(mm_tn(mlp_rows_in, grad_gate_b).astype(bf16), "ctx").astype(f32)
    up_sum = lax.psum(mm_tn(mlp_rows_in, grad_up_b).astype(bf16), "ctx").astype(f32)
    back_part = mm_nt(grad_gate_b, w_gate) + mm_nt(grad_up_b, w_up)
    grad_res = grad_y + reduce_line(back_part.reshape(owners, rows, width), 11)
    grad_proj, gain_attn = norm_back(projected, proj_scale, gains[2], grad_res)
    grad_proj_rows = gather_line(grad_proj.astype(bf16), 12)
    grad_mixed = mm_nt(grad_proj_rows, w_output).astype(bf16)
    (grad_mixed,) = exchange("ctx", [grad_mixed.reshape(parts, pair, rows, own_width)], 13)
    grad_queries, grad_keys, grad_values = exchange(
        "ctx", attend_back(packed, query_pos, key_pos, grad_mixed), 14
    )
    grad_queries = rope_back(grad_queries.reshape(group, own_width), cosine, sine)
    grad_keys = rope_back(grad_keys.reshape(group, own_width), cosine, sine)
    grad_value_b = grad_values.reshape(group, own_width)
    query_weighted, key_weighted = grad_queries * own_gains[0], grad_keys * own_gains[1]
    products = jnp.stack(
        [jnp.sum(query_weighted * query_raw, axis=-1), jnp.sum(key_weighted * key_raw, axis=-1)]
    )
    (products,) = exchange("fsdp", [products], 15, scatter=False)
    means = jnp.sum(products, axis=0) / width
    grad_query_b = (
        query_scale * query_weighted - query_raw * (query_scale**3 * means[0][:, None])
    ).astype(bf16)
    grad_key_b = (
        key_scale * key_weighted - key_raw * (key_scale**3 * means[1][:, None])
    ).astype(bf16)
    gain_query = jnp.sum(grad_queries * (query_raw * query_scale), axis=0)
    gain_key = jnp.sum(grad_keys * (key_raw * key_scale), axis=0)
    grad_heads = jnp.concatenate([grad_query_b, grad_key_b, grad_value_b], axis=1)
    input_grad = grad_res + reduce_line(
        mm_nt(grad_heads, w_heads).reshape(owners, rows, width), 16
    )

    (gain_post,) = exchange(
        "fsdp",
        [jnp.stack([gain_attn, gain_ff]).reshape(2, owners, own_width).transpose(1, 0, 2)],
        17,
    )
    gain_own = jnp.concatenate(
        [gain_query[None], gain_key[None], jnp.sum(gain_post, axis=0)], axis=0
    )
    (gain_own,) = exchange("ctx", [gain_own], 18, scatter=False)
    gain_own = jnp.sum(gain_own, axis=0)

    output_sum = lax.psum(
        mm_tn(mixed_group.reshape(owners, rows, own_width).reshape(group, own_width), grad_proj_rows).astype(bf16),
        "ctx",
    ).astype(f32)
    heads_part = (
        mm_tn(group_tokens, grad_heads)
        .astype(bf16)
        .reshape(owners, parts, piece, 3 * own_width)
        .transpose(1, 0, 2, 3)
    )
    heads_part = lax.psum_scatter(heads_part, "ctx", scatter_dimension=0, tiled=False)
    (heads_part,) = exchange("fsdp", [heads_part], 19)
    heads_all = lax.all_gather(heads_part, "ctx", axis=0)
    heads_all = (
        heads_all.reshape(parts, owners, piece, 3, own_width)
        .transpose(3, 0, 2, 1, 4)
        .reshape(3, parts * piece, width)
        .astype(f32)
    )
    return (
        block_out.astype(bf16)[None],
        input_grad[None],
        heads_all[0],
        heads_all[1],
        heads_all[2],
        output_sum,
        gate_sum,
        up_sum,
        down_sum,
        gain_own,
    )


def solution(mesh):
    return jax.shard_map(
        shards,
        mesh=mesh,
        in_specs=(
            P("fsdp", "ctx", None),
            P("fsdp", None),
            P("fsdp", None),
            P("fsdp", None),
            P("fsdp", None),
            P("fsdp", None),
            P(None, "fsdp"),
            P(None, "fsdp"),
            P("fsdp", None),
            P(None, "fsdp"),
            P("fsdp", "ctx", None),
        ),
        out_specs=(
            P("fsdp", "ctx", None),
            P("fsdp", "ctx", None),
            P("fsdp", None),
            P("fsdp", None),
            P("fsdp", None),
            P("fsdp", None),
            P(None, "fsdp"),
            P(None, "fsdp"),
            P("fsdp", None),
            P(None, "fsdp"),
        ),
        check_vma=False,
    )
```

```python
import functools

import jax
import jax.numpy as jnp
import numpy as np
from jax import lax
from jax.experimental import pallas as pl
from jax.experimental.pallas import tpu as pltpu
from jax.sharding import PartitionSpec as P

HEADS = 16
HEAD_DIM = 128

norm_eps = 1e-06
rope_base = 500000.0
neg_fill = -1e30

MESH = pl.DeviceIdType.MESH
f32 = jnp.float32
bf16 = jnp.bfloat16


def anywhere():
    return pl.BlockSpec(memory_space=pl.ANY)


def in_vmem():
    return pl.BlockSpec(memory_space=pltpu.VMEM)


def lasting(microseconds):
    return pl.CostEstimate(
        flops=0, transcendentals=0, bytes_accessed=int(microseconds * 3_300_000)
    )


def remote(source, target, sent, landed, where):
    return pltpu.make_async_remote_copy(
        src_ref=source,
        dst_ref=target,
        send_sem=sent,
        recv_sem=landed,
        device_id=where,
        device_id_type=MESH,
    )


def exchange_kernel(axis, size, scatter, count, *refs):
    given, kept = refs[:count], refs[count : 2 * count]
    own_sem, send_sem, land_sem = refs[2 * count :]
    own = lax.axis_index(axis)
    barrier = pltpu.get_barrier_semaphore()
    for step in range(1, size):
        pl.semaphore_signal(
            barrier, inc=1, device_id={axis: lax.rem(own + step, size)}, device_id_type=MESH
        )
    local = []
    for item in range(count):
        source = given[item].at[own] if scatter else given[item]
        local.append(pltpu.make_async_copy(source, kept[item].at[own], own_sem.at[item]))
        local[-1].start()
    pl.semaphore_wait(barrier, size - 1)
    copies = []
    for step in range(1, size):
        peer = lax.rem(own + step, size)
        for item in range(count):
            source = given[item].at[peer] if scatter else given[item]
            copies.append(
                remote(
                    source,
                    kept[item].at[own],
                    send_sem.at[item, step],
                    land_sem.at[item, step],
                    {axis: peer},
                )
            )
            copies[-1].start()
    for copy in local:
        copy.wait()
    for copy in copies:
        copy.wait()


def exchange(axis, arrays, key, scatter=True, takes=6):
    size = lax.axis_size(axis)
    count = len(arrays)
    shapes = [
        jax.ShapeDtypeStruct(item.shape if scatter else (size,) + item.shape, item.dtype)
        for item in arrays
    ]
    return pl.pallas_call(
        functools.partial(exchange_kernel, axis, size, scatter, count),
        out_shape=shapes,
        in_specs=[in_vmem()] * count,
        out_specs=[anywhere()] * count,
        scratch_shapes=[
            pltpu.SemaphoreType.DMA((count,)),
            pltpu.SemaphoreType.DMA((count, size)),
            pltpu.SemaphoreType.DMA((count, size)),
        ],
        compiler_params=pltpu.CompilerParams(collective_id=key, has_side_effects=True),
        cost_estimate=lasting(takes),
        name=f"exchange_{axis}_{key}",
    )(*arrays)


def greet_line(own, chips):
    chip, core = own // 2, own % 2
    barrier = pltpu.get_barrier_semaphore()

    def greet(place):
        pl.semaphore_signal(barrier, inc=1, device_id={"fsdp": place}, device_id_type=MESH)

    greet(chip * 2 + 1 - core)

    @pl.when(chip > 0)
    def _():
        greet(own - 2)

    @pl.when(chip < chips - 1)
    def _():
        greet(own + 2)

    expected = 1 + jnp.minimum(chip, 1) + jnp.minimum(chips - 1 - chip, 1)
    pl.semaphore_wait(barrier, expected)


def pass_along(chips, given, kept, local, send_sem, land_sem, between=None):
    own = lax.axis_index("fsdp")
    chip, core = own // 2, own % 2
    sibling = chip * 2 + 1 - core

    def copy(source, place, way, step, target):
        return remote(
            source, kept.at[place], send_sem.at[way, step], land_sem.at[place], {"fsdp": target}
        )

    @pl.when(chip < chips - 1)
    def _():
        copy(given, own, 0, 0, own + 2).start()

    @pl.when(chip > 0)
    def _():
        copy(given, own, 1, 0, own - 2).start()

    copy(given, own, 2, 0, sibling).start()
    local.wait()
    result = between() if between else None
    for step in range(1, chips):
        from_left, from_right = own - 2 * step, own + 2 * step

        @pl.when(chip >= step)
        def _():
            copy(kept.at[from_left], from_left, 0, step, own).wait_recv()

            @pl.when(chip < chips - 1)
            def _():
                copy(kept.at[from_left], from_left, 0, step, own + 2).start()

            copy(kept.at[from_left], from_left, 2, step, sibling).start()

        @pl.when(chip + step < chips)
        def _():
            copy(kept.at[from_right], from_right, 1, step, own).wait_recv()

            @pl.when(chip > 0)
            def _():
                copy(kept.at[from_right], from_right, 1, step, own - 2).start()

            copy(kept.at[from_right], from_right, 3, step, sibling).start()

    for other in range(chips):
        place = other * 2 + 1 - core
        copy(kept.at[place], place, 2, 0, sibling).wait_recv()

    @pl.when(chip < chips - 1)
    def _():
        copy(given, own, 0, 0, own + 2).wait_send()

    @pl.when(chip > 0)
    def _():
        copy(given, own, 1, 0, own - 2).wait_send()

    copy(given, own, 2, 0, sibling).wait_send()
    for step in range(1, chips):
        from_left, from_right = own - 2 * step, own + 2 * step

        @pl.when(chip >= step)
        def _():
            @pl.when(chip < chips - 1)
            def _():
                copy(kept.at[from_left], from_left, 0, step, own + 2).wait_send()

            copy(kept.at[from_left], from_left, 2, step, sibling).wait_send()

        @pl.when(chip + step < chips)
        def _():
            @pl.when(chip > 0)
            def _():
                copy(kept.at[from_right], from_right, 1, step, own - 2).wait_send()

            copy(kept.at[from_right], from_right, 3, step, sibling).wait_send()
    return result


def gather_kernel(chips, given, kept, own_sem, send_sem, land_sem):
    own = lax.axis_index("fsdp")
    local = pltpu.make_async_copy(given, kept.at[own], own_sem)
    local.start()
    greet_line(own, chips)
    pass_along(chips, given, kept, local, send_sem, land_sem)


def gather_line(shard, key):
    size = lax.axis_size("fsdp")
    chips = size // 2
    kept = pl.pallas_call(
        functools.partial(gather_kernel, chips),
        out_shape=jax.ShapeDtypeStruct((size,) + shard.shape, shard.dtype),
        in_specs=[in_vmem()],
        out_specs=anywhere(),
        scratch_shapes=[
            pltpu.SemaphoreType.DMA,
            pltpu.SemaphoreType.DMA((4, chips)),
            pltpu.SemaphoreType.DMA((size,)),
        ],
        compiler_params=pltpu.CompilerParams(collective_id=key, has_side_effects=True),
        cost_estimate=lasting(40),
        name=f"gather_line_{key}",
    )(shard)
    return kept.reshape((size * shard.shape[0],) + shard.shape[1:])


def reduce_kernel(
    chips,
    wire,
    given,
    total,
    mine,
    beside,
    from_left,
    from_right,
    outgoing,
    load_sem,
    side_send,
    side_land,
    line_send,
    left_land,
    right_land,
):
    own = lax.axis_index("fsdp")
    chip, core = own // 2, own % 2
    sibling = chip * 2 + 1 - core

    def load(other):
        return pltpu.make_async_copy(given.at[other * 2 + core], mine.at[other], load_sem.at[other])

    def side(other):
        return remote(
            given.at[other * 2 + 1 - core],
            beside.at[other],
            side_send.at[other],
            side_land.at[other],
            {"fsdp": sibling},
        )

    def rightward(other, target):
        return remote(
            outgoing.at[other],
            from_left.at[other],
            line_send.at[other],
            left_land.at[other],
            {"fsdp": target},
        )

    def leftward(other, target):
        return remote(
            outgoing.at[other],
            from_right.at[other],
            line_send.at[other],
            right_land.at[other],
            {"fsdp": target},
        )

    for other in range(chips):
        load(other).start()
    greet_line(own, chips)
    for tick in range(chips - 1):
        right_to = chips - 1 - (tick - chip)
        left_to = tick - (chips - 1 - chip)

        @pl.when((tick >= chip) & (right_to > chip))
        def _():
            side(right_to).start()

        @pl.when((left_to >= 0) & (left_to < chip))
        def _():
            side(left_to).start()

    side(chip).start()
    for tick in range(chips - 1):
        right_to = chips - 1 - (tick - chip)
        left_to = tick - (chips - 1 - chip)

        @pl.when((tick >= chip) & (right_to > chip))
        def _():
            load(right_to).wait()
            side(right_to).wait_recv()

            @pl.when(chip > 0)
            def _():
                rightward(right_to, own).wait_recv()
                outgoing[right_to] = (
                    mine[right_to] + beside[right_to] + from_left[right_to].astype(f32)
                ).astype(wire)

            @pl.when(chip == 0)
            def _():
                outgoing[right_to] = (mine[right_to] + beside[right_to]).astype(wire)

            rightward(right_to, own + 2).start()

        @pl.when((left_to >= 0) & (left_to < chip))
        def _():
            load(left_to).wait()
            side(left_to).wait_recv()

            @pl.when(chip < chips - 1)
            def _():
                leftward(left_to, own).wait_recv()
                outgoing[left_to] = (
                    mine[left_to] + beside[left_to] + from_right[left_to].astype(f32)
                ).astype(wire)

            @pl.when(chip == chips - 1)
            def _():
                outgoing[left_to] = (mine[left_to] + beside[left_to]).astype(wire)

            leftward(left_to, own - 2).start()

    load(chip).wait()
    side(chip).wait_recv()
    total[...] = mine[chip] + beside[chip]

    @pl.when(chip > 0)
    def _():
        rightward(chip, own).wait_recv()
        total[...] += from_left[chip].astype(f32)

    @pl.when(chip < chips - 1)
    def _():
        leftward(chip, own).wait_recv()
        total[...] += from_right[chip].astype(f32)

    for other in range(chips):
        side(other).wait_send()

        @pl.when(chip != other)
        def _():
            rightward(other, own).wait_send()


def reduce_line(partial, key, wire=f32):
    size, rows, width = partial.shape
    chips = size // 2
    return pl.pallas_call(
        functools.partial(reduce_kernel, chips, wire),
        out_shape=jax.ShapeDtypeStruct((rows, width), f32),
        in_specs=[anywhere()],
        out_specs=in_vmem(),
        scratch_shapes=[
            pltpu.VMEM((chips, rows, width), f32),
            pltpu.VMEM((chips, rows, width), f32),
            pltpu.VMEM((chips, rows, width), wire),
            pltpu.VMEM((chips, rows, width), wire),
            pltpu.VMEM((chips, rows, width), wire),
            pltpu.SemaphoreType.DMA((chips,)),
            pltpu.SemaphoreType.DMA((chips,)),
            pltpu.SemaphoreType.DMA((chips,)),
            pltpu.SemaphoreType.DMA((chips,)),
            pltpu.SemaphoreType.DMA((chips,)),
            pltpu.SemaphoreType.DMA((chips,)),
        ],
        compiler_params=pltpu.CompilerParams(
            collective_id=key, has_side_effects=True, vmem_limit_bytes=60 * 1024 * 1024
        ),
        cost_estimate=lasting(78 if wire == f32 else 42),
        name=f"reduce_line_{key}",
    )(partial)


def greet_peers(axes):
    barrier = pltpu.get_barrier_semaphore()
    expected = 0
    for axis in axes:
        own, size = lax.axis_index(axis), lax.axis_size(axis)
        for step in range(1, size):
            pl.semaphore_signal(
                barrier, inc=1, device_id={axis: lax.rem(own + step, size)}, device_id_type=MESH
            )
        expected += size - 1
    pl.semaphore_wait(barrier, expected)


def start_kernel(
    owners,
    parts,
    tokens,
    small,
    inverse,
    w_query,
    w_key,
    w_value,
    group_tokens,
    small_all,
    heads_w,
    cosines,
    sines,
    own_sem,
    small_send,
    small_land,
    piece_send,
    piece_land,
    part_send,
    part_land,
    line_send,
    line_land,
):
    own, part = lax.axis_index("fsdp"), lax.axis_index("ctx")
    piece, own_width = heads_w.shape[2], heads_w.shape[3] // 3
    weights = (w_query, w_key, w_value)

    def cut(item, place):
        return weights[item].at[
            pl.ds(pl.multiple_of(part * piece, piece), piece),
            pl.ds(pl.multiple_of(place * own_width, own_width), own_width),
        ]

    def slot(item, place):
        return heads_w.at[place, part, :, pl.ds(item * own_width, own_width)]

    local_tokens = pltpu.make_async_copy(tokens, group_tokens.at[own], own_sem.at[0])
    local_small = pltpu.make_async_copy(small, small_all.at[own], own_sem.at[1])
    local_pieces = [
        pltpu.make_async_copy(cut(item, own), slot(item, own), own_sem.at[2 + item])
        for item in range(3)
    ]
    for copy in [local_tokens, local_small] + local_pieces:
        copy.start()
    greet_peers(("fsdp", "ctx"))
    first = []
    for step in range(1, owners):
        peer = lax.rem(own + step, owners)
        for item in range(3):
            first.append(
                remote(
                    cut(item, peer),
                    slot(item, own),
                    piece_send.at[item, step],
                    piece_land.at[item, step],
                    {"fsdp": peer},
                )
            )
        first.append(
            remote(
                small,
                small_all.at[own],
                small_send.at[step],
                small_land.at[step],
                {"fsdp": peer},
            )
        )
    for copy in first:
        copy.start()
    for copy in [local_small] + local_pieces:
        copy.wait()

    seq_rows = cosines.shape[0]
    angle = (
        lax.broadcasted_iota(jnp.int32, (seq_rows, HEAD_DIM), 0).astype(f32) * inverse[...]
    )
    cosines[...] = jnp.cos(angle)
    lane = lax.broadcasted_iota(jnp.int32, (seq_rows, HEAD_DIM), 1)
    sines[...] = jnp.sin(angle) * jnp.where(lane < HEAD_DIM // 2, -1.0, 1.0)

    def relay():
        for copy in first:
            copy.wait_recv()
        second = []
        for step in range(1, parts):
            second.append(
                remote(
                    heads_w.at[:, part],
                    heads_w.at[:, part],
                    part_send.at[step],
                    part_land.at[step],
                    {"ctx": lax.rem(part + step, parts)},
                )
            )
            second[-1].start()
        return second

    second = pass_along(
        owners // 2, tokens, group_tokens, local_tokens, line_send, line_land, relay
    )
    for copy in first:
        copy.wait_send()
    for copy in second:
        copy.wait()


def start(tokens, small, weights, parts, owners):
    rows, width = tokens.shape
    own_width = width // owners
    piece = weights[0].shape[0] // parts
    inverse = rope_base ** (-(np.arange(HEAD_DIM // 2, dtype=np.float32) * 2.0) / HEAD_DIM)
    inverse = jnp.asarray(np.concatenate([inverse, inverse])[None], f32)
    chips = owners // 2
    return pl.pallas_call(
        functools.partial(start_kernel, owners, parts),
        out_shape=[
            jax.ShapeDtypeStruct((owners, rows, width), bf16),
            jax.ShapeDtypeStruct((owners,) + small.shape, f32),
            jax.ShapeDtypeStruct((owners, parts, piece, 3 * own_width), bf16),
            jax.ShapeDtypeStruct((parts * rows, HEAD_DIM), f32),
            jax.ShapeDtypeStruct((parts * rows, HEAD_DIM), f32),
        ],
        in_specs=[in_vmem(), in_vmem(), in_vmem(), anywhere(), anywhere(), anywhere()],
        out_specs=[anywhere(), anywhere(), anywhere(), in_vmem(), in_vmem()],
        scratch_shapes=[
            pltpu.SemaphoreType.DMA((5,)),
            pltpu.SemaphoreType.DMA((owners,)),
            pltpu.SemaphoreType.DMA((owners,)),
            pltpu.SemaphoreType.DMA((3, owners)),
            pltpu.SemaphoreType.DMA((3, owners)),
            pltpu.SemaphoreType.DMA((parts,)),
            pltpu.SemaphoreType.DMA((parts,)),
            pltpu.SemaphoreType.DMA((4, chips)),
            pltpu.SemaphoreType.DMA((owners,)),
        ],
        compiler_params=pltpu.CompilerParams(collective_id=0, has_side_effects=True),
        cost_estimate=lasting(60),
        name="start",
    )(tokens, small, inverse, *weights)


def as_row(column):
    rows = column.shape[0]
    return jnp.broadcast_to(column, (rows, 128)).T[:1]


def as_column(row):
    rows = row.shape[1]
    return jnp.broadcast_to(row, (128, rows)).T[:, :1]


def share_stats(stats, everyone, send_sem, land_sem):
    own, owners = lax.axis_index("fsdp"), lax.axis_size("fsdp")
    copies = []
    for step in range(1, owners):
        copies.append(
            remote(
                stats,
                everyone.at[own],
                send_sem.at[step],
                land_sem.at[step],
                {"fsdp": lax.rem(own + step, owners)},
            )
        )
        copies[-1].start()
    everyone[own] = stats[...]
    for copy in copies:
        copy.wait()
    total = everyone[0]
    for place in range(1, owners):
        total += everyone[place]
    return total


def table_rows(table, row_block, rows, block_rows):
    def block(at):
        taken = table[at * block_rows : (at + 1) * block_rows]
        return jnp.concatenate([taken] * (rows // block_rows), axis=0)

    found = block(0)
    for at in range(1, table.shape[0] // block_rows):
        found = jnp.where(row_block == at, block(at), found)
    return found


def each_head(width):
    return [slice(at, at + HEAD_DIM) for at in range(0, width, HEAD_DIM)]


def heads_kernel(
    block_rows,
    row_blocks,
    tokens,
    weights,
    cosines,
    sines,
    gains,
    packed,
    raw,
    scales,
    stage,
    stats,
    everyone,
    own_sem,
    stat_send,
    stat_land,
    part_send,
    part_land,
):
    owners, rows, width = tokens.shape
    parts, own_width = stage.shape[0], stage.shape[-1]
    pair = owners // parts
    part = lax.axis_index("ctx")
    greet_peers(("fsdp", "ctx"))

    def project(seq, carry):
        product = jnp.dot(tokens[seq], weights[...], preferred_element_type=f32)
        for kind in range(2):
            values = product[:, kind * own_width : (kind + 1) * own_width]
            raw[kind, seq] = values
            stats[pl.ds(kind * owners + seq, 1), :] = as_row(
                jnp.sum(values * values, axis=-1, keepdims=True)
            )
        stage[seq // pair, 2, seq % pair] = product[:, 2 * own_width :].astype(bf16)
        return carry

    lax.fori_loop(0, owners, project, 0)
    scales[...] = lax.rsqrt(share_stats(stats, everyone, stat_send, stat_land) / width + norm_eps)

    def rotate(seq, carry):
        row_block = row_blocks[seq]
        cosine = table_rows(cosines, row_block, rows, block_rows)
        sine = table_rows(sines, row_block, rows, block_rows)
        for kind in range(2):
            scale = as_column(scales[pl.ds(kind * owners + seq, 1), :])
            for head in each_head(own_width):
                values = raw[kind, seq, :, head] * scale * gains[kind : kind + 1, head]
                stage[seq // pair, kind, seq % pair, :, head] = (
                    values * cosine + pltpu.roll(values, HEAD_DIM // 2, 1) * sine
                ).astype(bf16)
        return carry

    copies = []
    for step in range(1, parts + 1):
        peer = lax.rem(part + step, parts)
        lax.fori_loop(peer * pair, (peer + 1) * pair, rotate, 0)
        if step < parts:
            copies.append(
                remote(
                    stage.at[peer],
                    packed.at[part],
                    part_send.at[step],
                    part_land.at[step],
                    {"ctx": peer},
                )
            )
        else:
            copies.append(pltpu.make_async_copy(stage.at[part], packed.at[part], own_sem))
        copies[-1].start()
    for copy in copies:
        copy.wait()


def heads(row_blocks, tokens, weights, cosines, sines, gains, parts, block_rows):
    owners, rows, width = tokens.shape
    own_width = width // owners
    pair = owners // parts
    packed = (parts, 3, pair, rows, own_width)
    return pl.pallas_call(
        functools.partial(heads_kernel, block_rows),
        out_shape=[
            jax.ShapeDtypeStruct(packed, bf16),
            jax.ShapeDtypeStruct((2, owners, rows, own_width), f32),
            jax.ShapeDtypeStruct((2 * owners, rows), f32),
        ],
        in_specs=[in_vmem()] * 6,
        out_specs=[anywhere(), in_vmem(), in_vmem()],
        scratch_shapes=[
            pltpu.VMEM(packed, bf16),
            pltpu.VMEM((2 * owners, rows), f32),
            pltpu.VMEM((owners, 2 * owners, rows), f32),
            pltpu.SemaphoreType.DMA,
            pltpu.SemaphoreType.DMA((owners,)),
            pltpu.SemaphoreType.DMA((owners,)),
            pltpu.SemaphoreType.DMA((parts,)),
            pltpu.SemaphoreType.DMA((parts,)),
        ],
        compiler_params=pltpu.CompilerParams(
            collective_id=1, has_side_effects=True, vmem_limit_bytes=60 * 1024 * 1024
        ),
        cost_estimate=lasting(35),
        name="heads",
    )(row_blocks, tokens, weights, cosines, sines, gains)


def heads_back_kernel(
    block_rows,
    row_blocks,
    grad_query,
    grad_key,
    grad_value,
    cosines,
    sines,
    gains,
    raw,
    scales,
    grads,
    gain_sums,
    pair_grads,
    pair_values,
    stats,
    everyone,
    own_sem,
    stat_send,
    stat_land,
    part_send,
    part_land,
):
    kinds, owners, rows, own_width = raw.shape
    parts = pair_values.shape[0]
    pair = owners // parts
    width = owners * own_width
    part = lax.axis_index("ctx")
    sources = (grad_query, grad_key, grad_value)

    def landing(item, place):
        return pair_values.at[place] if item == 2 else pair_grads.at[item, place]

    local = [
        pltpu.make_async_copy(sources[item].at[part], landing(item, part), own_sem.at[item])
        for item in range(3)
    ]
    for copy in local:
        copy.start()
    greet_peers(("fsdp", "ctx"))
    copies = []
    for step in range(1, parts):
        peer = lax.rem(part + step, parts)
        for item in range(3):
            copies.append(
                remote(
                    sources[item].at[peer],
                    landing(item, part),
                    part_send.at[item, step],
                    part_land.at[item, step],
                    {"ctx": peer},
                )
            )
            copies[-1].start()
    gain_sums[...] = jnp.zeros_like(gain_sums)
    for copy in local:
        copy.wait()
    for copy in copies:
        copy.wait()

    def unrotate(seq, carry):
        row_block = row_blocks[seq]
        cosine = table_rows(cosines, row_block, rows, block_rows)
        sine = table_rows(sines, row_block, rows, block_rows)
        for kind in range(kinds):
            scale = as_column(scales[pl.ds(kind * owners + seq, 1), :])
            products = jnp.zeros((rows, 1), f32)
            for head in each_head(own_width):
                rotated = pair_grads[kind, seq // pair, seq % pair, :, head]
                values = rotated * cosine - pltpu.roll(rotated, HEAD_DIM // 2, 1) * sine
                plain = raw[kind, seq, :, head]
                gain_sums[kind : kind + 1, head] += jnp.sum(
                    values * (plain * scale), axis=0, keepdims=True
                )
                values = values * gains[kind : kind + 1, head]
                pair_grads[kind, seq // pair, seq % pair, :, head] = values
                products += jnp.sum(values * plain, axis=-1, keepdims=True)
            stats[pl.ds(kind * owners + seq, 1), :] = as_row(products)
        return carry

    lax.fori_loop(0, owners, unrotate, 0)
    means = share_stats(stats, everyone, stat_send, stat_land) / width
    stats[...] = means

    def through_norm(seq, carry):
        for kind in range(kinds):
            row = pl.ds(kind * owners + seq, 1)
            scale, mean = as_column(scales[row, :]), as_column(stats[row, :])
            grads[seq, :, kind * own_width : (kind + 1) * own_width] = (
                scale * pair_grads[kind, seq // pair, seq % pair]
                - raw[kind, seq] * (scale * scale * scale * mean)
            ).astype(bf16)
        grads[seq, :, 2 * own_width :] = pair_values[seq // pair, seq % pair]
        return carry

    lax.fori_loop(0, owners, through_norm, 0)


def heads_back(row_blocks, pair_grads, cosines, sines, gains, raw, scales, block_rows):
    kinds, owners, rows, own_width = raw.shape
    parts, pair = pair_grads[0].shape[:2]
    return pl.pallas_call(
        functools.partial(heads_back_kernel, block_rows),
        out_shape=[
            jax.ShapeDtypeStruct((owners, rows, 3 * own_width), bf16),
            jax.ShapeDtypeStruct((2, own_width), f32),
        ],
        in_specs=[in_vmem()] * 9,
        out_specs=[in_vmem(), in_vmem()],
        scratch_shapes=[
            pltpu.VMEM((2, parts, pair, rows, own_width), f32),
            pltpu.VMEM((parts, pair, rows, own_width), bf16),
            pltpu.VMEM((2 * owners, rows), f32),
            pltpu.VMEM((owners, 2 * owners, rows), f32),
            pltpu.SemaphoreType.DMA((3,)),
            pltpu.SemaphoreType.DMA((owners,)),
            pltpu.SemaphoreType.DMA((owners,)),
            pltpu.SemaphoreType.DMA((3, parts)),
            pltpu.SemaphoreType.DMA((3, parts)),
        ],
        compiler_params=pltpu.CompilerParams(
            collective_id=2, has_side_effects=True, vmem_limit_bytes=60 * 1024 * 1024
        ),
        cost_estimate=lasting(45),
        name="heads_back",
    )(row_blocks, *pair_grads, cosines, sines, gains, raw, scales)


def finish_kernel(
    owners,
    parts,
    sums,
    gain_post,
    gain_heads,
    kept,
    gain_own,
    post_all,
    gain_mine,
    part_all,
    own_sem,
    piece_send,
    piece_land,
    part_send,
    part_land,
    post_send,
    post_land,
    gain_send,
    gain_land,
):
    own, part = lax.axis_index("fsdp"), lax.axis_index("ctx")
    width = kept.shape[3]
    own_width = width // owners

    def cut(item, place):
        start = pl.multiple_of((place * 3 + item) * own_width, own_width)
        return sums.at[:, pl.ds(start, own_width)]

    def slot(item):
        return kept.at[
            part, item, :, pl.ds(pl.multiple_of(own * own_width, own_width), own_width)
        ]

    output_rows = sums.at[:, pl.ds(3 * width, width)]
    local = [
        pltpu.make_async_copy(cut(item, own), slot(item), own_sem.at[item]) for item in range(3)
    ]
    local.append(pltpu.make_async_copy(output_rows, kept.at[part, 3], own_sem.at[3]))
    for copy in local:
        copy.start()
    greet_peers(("fsdp", "ctx"))
    first, posts, second = [], [], []
    for step in range(1, owners):
        peer = lax.rem(own + step, owners)
        for item in range(3):
            first.append(
                remote(
                    cut(item, peer),
                    slot(item),
                    piece_send.at[item, step],
                    piece_land.at[item, step],
                    {"fsdp": peer},
                )
            )
        posts.append(
            remote(
                gain_post.at[peer],
                post_all.at[own],
                post_send.at[step],
                post_land.at[step],
                {"fsdp": peer},
            )
        )
    for copy in first + posts:
        copy.start()
    for step in range(1, parts):
        second.append(
            remote(
                output_rows,
                kept.at[part, 3],
                part_send.at[0, step],
                part_land.at[0, step],
                {"ctx": lax.rem(part + step, parts)},
            )
        )
        second[-1].start()
    post_all[own] = gain_post[own]
    for copy in local:
        copy.wait()
    for copy in first:
        copy.wait_recv()
    for step in range(1, parts):
        second.append(
            remote(
                kept.at[part, pl.ds(0, 3)],
                kept.at[part, pl.ds(0, 3)],
                part_send.at[1, step],
                part_land.at[1, step],
                {"ctx": lax.rem(part + step, parts)},
            )
        )
        second[-1].start()
    for copy in posts:
        copy.wait()
    post = post_all[0]
    for place in range(1, owners):
        post += post_all[place]
    gain_mine[:2, :] = gain_heads[...]
    gain_mine[2:, :] = post
    gains = []
    for step in range(1, parts):
        gains.append(
            remote(
                gain_mine,
                part_all.at[part],
                gain_send.at[step],
                gain_land.at[step],
                {"ctx": lax.rem(part + step, parts)},
            )
        )
        gains[-1].start()
    part_all[part] = gain_mine[...]
    for copy in gains:
        copy.wait()
    total = part_all[0]
    for place in range(1, parts):
        total += part_all[place]
    gain_own[...] = total
    for copy in first:
        copy.wait_send()
    for copy in second:
        copy.wait()


def finish(sums, gain_post, gain_heads):
    owners, parts = lax.axis_size("fsdp"), lax.axis_size("ctx")
    piece, columns = sums.shape
    width = columns // 4
    own_width = width // owners
    return pl.pallas_call(
        functools.partial(finish_kernel, owners, parts),
        out_shape=[
            jax.ShapeDtypeStruct((parts, 4, piece, width), bf16),
            jax.ShapeDtypeStruct((4, own_width), f32),
        ],
        in_specs=[in_vmem(), in_vmem(), in_vmem()],
        out_specs=[anywhere(), in_vmem()],
        scratch_shapes=[
            pltpu.VMEM((owners, 2, own_width), f32),
            pltpu.VMEM((4, own_width), f32),
            pltpu.VMEM((parts, 4, own_width), f32),
            pltpu.SemaphoreType.DMA((4,)),
            pltpu.SemaphoreType.DMA((3, owners)),
            pltpu.SemaphoreType.DMA((3, owners)),
            pltpu.SemaphoreType.DMA((2, parts)),
            pltpu.SemaphoreType.DMA((2, parts)),
            pltpu.SemaphoreType.DMA((owners,)),
            pltpu.SemaphoreType.DMA((owners,)),
            pltpu.SemaphoreType.DMA((parts,)),
            pltpu.SemaphoreType.DMA((parts,)),
        ],
        compiler_params=pltpu.CompilerParams(collective_id=3, has_side_effects=True),
        cost_estimate=lasting(50),
        name="finish",
    )(sums, gain_post, gain_heads)


def probs_of(query, key, query_pos, key_pos):
    scores = lax.dot_general(
        query, key, (((1,), (1,)), ((), ())), preferred_element_type=f32
    ) * (HEAD_DIM ** (-0.5))
    scores = jnp.where(key_pos <= query_pos, scores, neg_fill)
    expd = jnp.exp(scores - jnp.max(scores, axis=-1, keepdims=True))
    return expd / jnp.sum(expd, axis=-1, keepdims=True)


def flat(ref):
    return ref[...].reshape(ref.shape[0] * ref.shape[-2], ref.shape[-1])


def attend_kernel(query_ref, key_ref, value_ref, query_pos, key_pos, mixed_ref):
    probs = probs_of(flat(query_ref), flat(key_ref), query_pos[...], key_pos[...])
    mixed_ref[...] = jnp.dot(
        probs.astype(bf16), flat(value_ref), preferred_element_type=f32
    ).astype(bf16)


def attend_back_kernel(
    query_ref,
    key_ref,
    value_ref,
    query_pos,
    key_pos,
    grad_ref,
    grad_query_ref,
    grad_key_ref,
    grad_value_ref,
    key_sum,
    value_sum,
):
    step, steps = pl.program_id(2), pl.num_programs(2)
    score_scale = HEAD_DIM ** (-0.5)
    query, key, value = flat(query_ref), flat(key_ref), flat(value_ref)
    grad = grad_ref[...]
    probs = probs_of(query, key, query_pos[...], key_pos[...])
    grad_probs = lax.dot_general(
        grad, value, (((1,), (1,)), ((), ())), preferred_element_type=f32
    )
    grad_scores = (
        probs * (grad_probs - jnp.sum(probs * grad_probs, axis=-1, keepdims=True))
    ).astype(bf16)
    grad_query_ref[...] = jnp.dot(grad_scores, key, preferred_element_type=f32) * score_scale
    value_part = lax.dot_general(
        probs.astype(bf16), grad, (((0,), (0,)), ((), ())), preferred_element_type=f32
    )
    key_part = lax.dot_general(
        grad_scores, query, (((0,), (0,)), ((), ())), preferred_element_type=f32
    )

    @pl.when(step == 0)
    def _():
        key_sum[...] = key_part
        value_sum[...] = value_part

    @pl.when(step > 0)
    def _():
        key_sum[...] += key_part
        value_sum[...] += value_part

    @pl.when(step == steps - 1)
    def _():
        grad_key_ref[...] = (key_sum[...] * score_scale).reshape(grad_key_ref.shape)
        grad_value_ref[...] = value_sum[...].astype(bf16).reshape(grad_value_ref.shape)


def attention_specs(parts, rows, seq_rows):
    query = pl.BlockSpec((1, None, None, rows, HEAD_DIM), lambda i, h, c: (c, 0, i, 0, h))
    key = pl.BlockSpec((parts, None, None, rows, HEAD_DIM), lambda i, h, c: (0, 1, i, 0, h))
    value = pl.BlockSpec((parts, None, None, rows, HEAD_DIM), lambda i, h, c: (0, 2, i, 0, h))
    query_pos = pl.BlockSpec((None, None, rows, 1), lambda i, h, c: (i, c, 0, 0))
    key_pos = pl.BlockSpec((None, 1, seq_rows), lambda i, h, c: (i, 0, 0))
    row_block = pl.BlockSpec((None, None, rows, HEAD_DIM), lambda i, h, c: (c, i, 0, h))
    all_block = pl.BlockSpec((parts, None, rows, HEAD_DIM), lambda i, h, c: (0, i, 0, h))
    return [query, key, value, query_pos, key_pos], row_block, all_block


def attend(packed, query_pos, key_pos):
    parts, _, pair, rows, width = packed.shape
    seq_rows = parts * rows
    in_specs, row_block, _ = attention_specs(parts, rows, seq_rows)
    return pl.pallas_call(
        attend_kernel,
        grid=(pair, width // HEAD_DIM, parts),
        out_shape=jax.ShapeDtypeStruct((parts, pair, rows, width), bf16),
        in_specs=in_specs,
        out_specs=row_block,
        cost_estimate=lasting(12),
        name="attend",
    )(packed, packed, packed, query_pos, key_pos)


def attend_back(packed, query_pos, key_pos, grad):
    parts, _, pair, rows, width = packed.shape
    seq_rows = parts * rows
    in_specs, row_block, all_block = attention_specs(parts, rows, seq_rows)
    return pl.pallas_call(
        attend_back_kernel,
        grid=(pair, width // HEAD_DIM, parts),
        out_shape=[
            jax.ShapeDtypeStruct((parts, pair, rows, width), f32),
            jax.ShapeDtypeStruct((parts, pair, rows, width), f32),
            jax.ShapeDtypeStruct((parts, pair, rows, width), bf16),
        ],
        in_specs=in_specs + [row_block],
        out_specs=[row_block, all_block, all_block],
        scratch_shapes=[
            pltpu.VMEM((seq_rows, HEAD_DIM), f32),
            pltpu.VMEM((seq_rows, HEAD_DIM), f32),
        ],
        cost_estimate=lasting(16),
        name="attend_back",
    )(packed, packed, packed, query_pos, key_pos, grad)


def norm_stat(values):
    return lax.rsqrt(jnp.mean(values * values, axis=-1, keepdims=True) + norm_eps)


def norm_back(values, scale, gain, grad_out):
    weighted = grad_out * gain
    grad_values = scale * weighted - values * (scale * scale * scale) * jnp.mean(
        weighted * values, axis=-1, keepdims=True
    )
    grad_gain = jnp.sum(grad_out * (values * scale), axis=0)
    return (grad_values, grad_gain)


def mm(left, right):
    return jnp.dot(left, right, preferred_element_type=f32)


def mm_nt(left, right):
    return lax.dot_general(left, right, (((1,), (1,)), ((), ())), preferred_element_type=f32)


def mm_tn(left, right):
    return lax.dot_general(left, right, (((0,), (0,)), ((), ())), preferred_element_type=f32)


def shards(
    hidden_in,
    block_order,
    w_query,
    w_key,
    w_value,
    w_output,
    w_gate,
    w_up,
    w_down,
    norm_gains,
    out_grad,
):
    rows, width = hidden_in.shape[1:]
    parts, owners = lax.axis_size("ctx"), lax.axis_size("fsdp")
    part = lax.axis_index("ctx")
    group = owners * rows
    own_width = width // owners
    pair = owners // parts
    blocks = block_order.shape[1]
    block_rows = parts * rows // blocks
    tokens_b = hidden_in[0]
    tokens_f = tokens_b.astype(f32)
    own_gains = norm_gains.astype(f32)

    small = jnp.concatenate(
        [own_gains, jnp.pad(block_order.astype(f32), ((0, 0), (0, own_width - blocks)))], axis=0
    )
    group_tokens, small_all, w_heads, cosines, sines = start(
        tokens_b, small, (w_query, w_key, w_value), parts, owners
    )
    w_heads = w_heads.reshape(width, 3 * own_width)
    group_tokens, w_output_in = lax.optimization_barrier((group_tokens, w_output))
    full_output = lax.all_gather(w_output_in, "fsdp", axis=0, tiled=True)
    gains = small_all[:, :4].transpose(1, 0, 2).reshape(4, width)
    orders = small_all[:, 4, :blocks].astype(jnp.int32)

    own_blocks = rows // block_rows
    row_blocks = jnp.repeat(
        lax.dynamic_slice_in_dim(orders, part * own_blocks, own_blocks, 1), block_rows, axis=1
    )[:, :, None]
    packed, raw, scales = heads(
        row_blocks, group_tokens, w_heads, cosines, sines, own_gains[:2], parts, block_rows
    )
    offsets = jnp.arange(block_rows, dtype=jnp.int32)
    pair_orders = lax.dynamic_slice_in_dim(orders, part * pair, pair, 0)
    pair_pos = pair_orders[:, :, None] * block_rows + offsets[None, None, :]
    query_pos = pair_pos.reshape(pair, parts, rows, 1)
    key_pos = pair_pos.reshape(pair, 1, parts * rows)
    mixed_pair = attend(packed, query_pos, key_pos)
    (mixed_group,) = exchange("ctx", [mixed_pair], 6, takes=10)
    mixed_group = mixed_group.reshape(owners, rows, own_width)
    (mixed_own,) = exchange("fsdp", [mixed_group], 7, takes=14)
    mixed_own = mixed_own.transpose(1, 0, 2).reshape(rows, width)
    projected = mm(mixed_own, full_output)
    proj_scale = norm_stat(projected)
    residual = tokens_f + projected * proj_scale * gains[2]
    mlp_rows_in = gather_line(residual.astype(bf16), 8)
    gate = mm(mlp_rows_in, w_gate)
    upward = mm(mlp_rows_in, w_up)
    sigma = jax.nn.sigmoid(gate)
    hidden_b = (gate * sigma * upward).astype(bf16)
    mlp_out = reduce_line(mm(hidden_b, w_down).reshape(owners, rows, width), 9, wire=bf16)
    mlp_scale = norm_stat(mlp_out)
    block_out = residual + mlp_out * mlp_scale * gains[3]

    grad_y = out_grad[0].astype(f32)
    grad_mlp, gain_ff = norm_back(mlp_out, mlp_scale, gains[3], grad_y)
    grad_rows = gather_line(grad_mlp.astype(bf16), 10)
    grad_rows, down_part = lax.optimization_barrier(
        (grad_rows, mm_tn(hidden_b, grad_rows).astype(bf16))
    )
    grad_hidden = mm_nt(grad_rows, w_down)
    grad_gate_b = (grad_hidden * upward * sigma * (1.0 + gate * (1.0 - sigma))).astype(bf16)
    grad_up_b = (grad_hidden * (gate * sigma)).astype(bf16)
    grad_gate_b, grad_up_b, gate_part, up_part = lax.optimization_barrier(
        (
            grad_gate_b,
            grad_up_b,
            mm_tn(mlp_rows_in, grad_gate_b).astype(bf16),
            mm_tn(mlp_rows_in, grad_up_b).astype(bf16),
        )
    )
    down_sum, gate_sum, up_sum = lax.psum((down_part, gate_part, up_part), "ctx")
    back_part = mm_nt(grad_gate_b, w_gate) + mm_nt(grad_up_b, w_up)
    grad_res = grad_y + reduce_line(back_part.reshape(owners, rows, width), 11, wire=bf16)
    grad_proj, gain_attn = norm_back(projected, proj_scale, gains[2], grad_res)
    grad_proj_rows = gather_line(grad_proj.astype(bf16), 12)
    grad_mixed = mm_nt(grad_proj_rows, w_output).astype(bf16)
    (grad_mixed,) = exchange(
        "ctx", [grad_mixed.reshape(parts, pair, rows, own_width)], 13, takes=10
    )
    pair_grads = attend_back(packed, query_pos, key_pos, grad_mixed)
    grad_heads, gain_heads = heads_back(
        row_blocks, pair_grads, cosines, sines, own_gains[:2], raw, scales, block_rows
    )
    grad_heads = grad_heads.reshape(group, 3 * own_width)

    piece = own_width // parts
    output_part = mm_tn(mixed_group.reshape(group, own_width), grad_proj_rows).astype(bf16)
    heads_part = mm_tn(group_tokens.reshape(group, width), grad_heads).astype(bf16)
    attention_part = jnp.concatenate(
        [
            heads_part.reshape(owners, parts, piece, 3 * own_width)
            .transpose(1, 2, 0, 3)
            .reshape(parts, piece, 3 * width),
            output_part.reshape(parts, piece, width),
        ],
        axis=2,
    )
    attention_part, down_sum, gate_sum, up_sum = lax.optimization_barrier(
        (attention_part, down_sum, gate_sum, up_sum)
    )
    attention_part = lax.psum_scatter(attention_part, "ctx", scatter_dimension=0, tiled=False)
    input_grad = grad_res + reduce_line(
        mm_nt(grad_heads, w_heads).reshape(owners, rows, width), 16, wire=bf16
    )
    attention_part, input_grad = lax.optimization_barrier((attention_part, input_grad))
    gain_post = jnp.stack([gain_attn, gain_ff]).reshape(2, owners, own_width).transpose(1, 0, 2)
    attention_all, gain_own = finish(attention_part, gain_post, gain_heads)
    attention_all = [
        attention_all[:, item].reshape(own_width, width).astype(f32) for item in range(4)
    ]
    return (
        block_out.astype(bf16)[None],
        input_grad[None],
        *attention_all,
        gate_sum.astype(f32),
        up_sum.astype(f32),
        down_sum.astype(f32),
        gain_own,
    )


def solution(mesh):
    return jax.shard_map(
        shards,
        mesh=mesh,
        in_specs=(
            P("fsdp", "ctx", None),
            P("fsdp", None),
            P("fsdp", None),
            P("fsdp", None),
            P("fsdp", None),
            P("fsdp", None),
            P(None, "fsdp"),
            P(None, "fsdp"),
            P("fsdp", None),
            P(None, "fsdp"),
            P("fsdp", "ctx", None),
        ),
        out_specs=(
            P("fsdp", "ctx", None),
            P("fsdp", "ctx", None),
            P("fsdp", None),
            P("fsdp", None),
            P("fsdp", None),
            P("fsdp", None),
            P(None, "fsdp"),
            P(None, "fsdp"),
            P("fsdp", None),
            P(None, "fsdp"),
        ),
        check_vma=False,
    )
```

```python
import functools

import jax
import jax.numpy as jnp
import numpy as np
from jax import lax
from jax.experimental import pallas as pl
from jax.experimental.pallas import tpu as pltpu
from jax.sharding import PartitionSpec as P

HEADS = 16
HEAD_DIM = 128

norm_eps = 1e-06
rope_base = 500000.0
neg_fill = -1e30

MESH = pl.DeviceIdType.MESH
f32 = jnp.float32
bf16 = jnp.bfloat16


def anywhere():
    return pl.BlockSpec(memory_space=pl.ANY)


def in_vmem():
    return pl.BlockSpec(memory_space=pltpu.VMEM)


def lasting(microseconds):
    return pl.CostEstimate(
        flops=0, transcendentals=0, bytes_accessed=int(microseconds * 3_300_000)
    )


def remote(source, target, sent, landed, where):
    return pltpu.make_async_remote_copy(
        src_ref=source,
        dst_ref=target,
        send_sem=sent,
        recv_sem=landed,
        device_id=where,
        device_id_type=MESH,
    )


def exchange_kernel(axis, size, scatter, count, *refs):
    given, kept = refs[:count], refs[count : 2 * count]
    own_sem, send_sem, land_sem = refs[2 * count :]
    own = lax.axis_index(axis)
    barrier = pltpu.get_barrier_semaphore()
    for step in range(1, size):
        pl.semaphore_signal(
            barrier, inc=1, device_id={axis: lax.rem(own + step, size)}, device_id_type=MESH
        )
    local = []
    for item in range(count):
        source = given[item].at[own] if scatter else given[item]
        local.append(pltpu.make_async_copy(source, kept[item].at[own], own_sem.at[item]))
        local[-1].start()
    pl.semaphore_wait(barrier, size - 1)
    copies = []
    for step in range(1, size):
        peer = lax.rem(own + step, size)
        for item in range(count):
            source = given[item].at[peer] if scatter else given[item]
            copies.append(
                remote(
                    source,
                    kept[item].at[own],
                    send_sem.at[item, step],
                    land_sem.at[item, step],
                    {axis: peer},
                )
            )
            copies[-1].start()
    for copy in local:
        copy.wait()
    for copy in copies:
        copy.wait()


def exchange(axis, arrays, key, scatter=True, takes=6):
    size = lax.axis_size(axis)
    count = len(arrays)
    shapes = [
        jax.ShapeDtypeStruct(item.shape if scatter else (size,) + item.shape, item.dtype)
        for item in arrays
    ]
    return pl.pallas_call(
        functools.partial(exchange_kernel, axis, size, scatter, count),
        out_shape=shapes,
        in_specs=[in_vmem()] * count,
        out_specs=[anywhere()] * count,
        scratch_shapes=[
            pltpu.SemaphoreType.DMA((count,)),
            pltpu.SemaphoreType.DMA((count, size)),
            pltpu.SemaphoreType.DMA((count, size)),
        ],
        compiler_params=pltpu.CompilerParams(collective_id=key, has_side_effects=True),
        cost_estimate=lasting(takes),
        name=f"exchange_{axis}_{key}",
    )(*arrays)


def greet_line(own, chips):
    chip, core = own // 2, own % 2
    barrier = pltpu.get_barrier_semaphore()

    def greet(place):
        pl.semaphore_signal(barrier, inc=1, device_id={"fsdp": place}, device_id_type=MESH)

    greet(chip * 2 + 1 - core)

    @pl.when(chip > 0)
    def _():
        greet(own - 2)

    @pl.when(chip < chips - 1)
    def _():
        greet(own + 2)

    expected = 1 + jnp.minimum(chip, 1) + jnp.minimum(chips - 1 - chip, 1)
    pl.semaphore_wait(barrier, expected)


CUTS = 4


def pass_along(chips, given, kept, local, send_sem, land_sem, between=None, use=None):
    own = lax.axis_index("fsdp")
    chip, core = own // 2, own % 2
    sibling = chip * 2 + 1 - core
    height = given.shape[0] // CUTS

    def copy(source, place, way, step, cut, target):
        rows = pl.ds(cut * height, height)
        return remote(
            source.at[rows],
            kept.at[place, rows],
            send_sem.at[way, step, cut],
            land_sem.at[place, cut],
            {"fsdp": target},
        )

    def both_ways(step, cut, left_does, right_does):
        from_left, from_right = own - 2 * step, own + 2 * step

        @pl.when(chip >= step)
        def _():
            left_does(from_left, step, cut)

        @pl.when(chip + step < chips)
        def _():
            right_does(from_right, step, cut)

    def hand_on(way, nearer, side):
        def does(place, step, cut):
            copy(kept.at[place], place, way, step, cut, own).wait_recv()

            @pl.when((chip < chips - 1) if way == 0 else (chip > 0))
            def _():
                copy(kept.at[place], place, way, step, cut, nearer).start()

            copy(kept.at[place], place, side, step, cut, sibling).start()

        return does

    def sent(way, nearer, side):
        def does(place, step, cut):
            @pl.when((chip < chips - 1) if way == 0 else (chip > 0))
            def _():
                copy(kept.at[place], place, way, step, cut, nearer).wait_send()

            copy(kept.at[place], place, side, step, cut, sibling).wait_send()

        return does

    def from_sibling(other):
        place = other * 2 + 1 - core
        for cut in range(CUTS):
            copy(kept.at[place], place, 2, 0, cut, sibling).wait_recv()
        if use:
            use(other)

    for cut in range(CUTS):

        @pl.when(chip < chips - 1)
        def _():
            copy(given, own, 0, 0, cut, own + 2).start()

        @pl.when(chip > 0)
        def _():
            copy(given, own, 1, 0, cut, own - 2).start()

        copy(given, own, 2, 0, cut, sibling).start()
    local.wait()
    result = between() if between else None
    from_sibling(chip)
    for step in range(1, chips):
        for cut in range(CUTS):
            both_ways(step, cut, hand_on(0, own + 2, 2), hand_on(1, own - 2, 3))

        @pl.when(chip >= step)
        def _():
            from_sibling(chip - step)

        @pl.when(chip + step < chips)
        def _():
            from_sibling(chip + step)

    for cut in range(CUTS):

        @pl.when(chip < chips - 1)
        def _():
            copy(given, own, 0, 0, cut, own + 2).wait_send()

        @pl.when(chip > 0)
        def _():
            copy(given, own, 1, 0, cut, own - 2).wait_send()

        copy(given, own, 2, 0, cut, sibling).wait_send()
        for step in range(1, chips):
            both_ways(step, cut, sent(0, own + 2, 2), sent(1, own - 2, 3))
    return result


def line_semaphores(owners):
    return [
        pltpu.SemaphoreType.DMA((4, owners // 2, CUTS)),
        pltpu.SemaphoreType.DMA((owners, CUTS)),
    ]


def gather_kernel(chips, given, kept, own_sem, send_sem, land_sem):
    own = lax.axis_index("fsdp")
    local = pltpu.make_async_copy(given, kept.at[own], own_sem)
    local.start()
    greet_line(own, chips)
    pass_along(chips, given, kept, local, send_sem, land_sem)


def gather_line(shard, key):
    size = lax.axis_size("fsdp")
    kept = pl.pallas_call(
        functools.partial(gather_kernel, size // 2),
        out_shape=jax.ShapeDtypeStruct((size,) + shard.shape, shard.dtype),
        in_specs=[in_vmem()],
        out_specs=anywhere(),
        scratch_shapes=[pltpu.SemaphoreType.DMA] + line_semaphores(size),
        compiler_params=pltpu.CompilerParams(collective_id=key, has_side_effects=True),
        cost_estimate=lasting(40),
        name=f"gather_line_{key}",
    )(shard)
    return kept.reshape((size * shard.shape[0],) + shard.shape[1:])


TILE = 512


def each_tile(columns, does):
    width = min(TILE, columns)

    def step(at, carry):
        does(pl.ds(pl.multiple_of(at * width, width), width))
        return carry

    lax.fori_loop(0, columns // width, step, 0)


def chip_rows(ref, other):
    taken = ref[pl.ds(other * 2, 2)]
    return taken.reshape(2 * taken.shape[1], taken.shape[2])


def put_chip(ref, other, columns, values):
    rows = ref.shape[1]
    ref[other * 2, :, columns] = values[:rows]
    ref[other * 2 + 1, :, columns] = values[rows:]


def ffn_in_kernel(
    chips,
    given,
    w_gate,
    w_up,
    rows_out,
    gate_out,
    up_out,
    hidden_out,
    rows,
    gate_w,
    up_w,
    gate,
    upward,
    hidden,
    own_sem,
    send_sem,
    land_sem,
    out_sem,
):
    own = lax.axis_index("fsdp")
    local = pltpu.make_async_copy(given, rows.at[own], own_sem.at[0])
    local.start()
    load = [
        pltpu.make_async_copy(w_gate, gate_w, own_sem.at[1]),
        pltpu.make_async_copy(w_up, up_w, own_sem.at[2]),
    ]
    for copy in load:
        copy.start()
    greet_line(own, chips)

    def stores(other):
        place = pl.ds(other * 2, 2)
        pairs = ((rows, rows_out), (gate, gate_out), (upward, up_out), (hidden, hidden_out))
        return [
            pltpu.make_async_copy(source.at[place], target.at[place], out_sem.at[item, other])
            for item, (source, target) in enumerate(pairs)
        ]

    def use(other):
        left = chip_rows(rows, other)

        def tile(columns):
            gated = jnp.dot(left, gate_w[:, columns], preferred_element_type=f32)
            raised = jnp.dot(left, up_w[:, columns], preferred_element_type=f32)
            put_chip(gate, other, columns, gated)
            put_chip(upward, other, columns, raised)
            put_chip(
                hidden, other, columns, (gated * jax.nn.sigmoid(gated) * raised).astype(bf16)
            )

        each_tile(gate_w.shape[1], tile)
        for copy in stores(other):
            copy.start()

    def loaded():
        for copy in load:
            copy.wait()

    pass_along(chips, given, rows, local, send_sem, land_sem, loaded, use)
    for other in range(chips):
        for copy in stores(other):
            copy.wait()


def ffn_in(shard, w_gate, w_up):
    owners = lax.axis_size("fsdp")
    rows, width = shard.shape
    units = w_gate.shape[1]
    wide, narrow = (owners, rows, width), (owners, rows, units)
    return pl.pallas_call(
        functools.partial(ffn_in_kernel, owners // 2),
        out_shape=[
            jax.ShapeDtypeStruct(wide, bf16),
            jax.ShapeDtypeStruct(narrow, f32),
            jax.ShapeDtypeStruct(narrow, f32),
            jax.ShapeDtypeStruct(narrow, bf16),
        ],
        in_specs=[in_vmem(), anywhere(), anywhere()],
        out_specs=[anywhere()] * 4,
        scratch_shapes=[
            pltpu.VMEM(wide, bf16),
            pltpu.VMEM((width, units), bf16),
            pltpu.VMEM((width, units), bf16),
            pltpu.VMEM(narrow, f32),
            pltpu.VMEM(narrow, f32),
            pltpu.VMEM(narrow, bf16),
            pltpu.SemaphoreType.DMA((3,)),
        ]
        + line_semaphores(owners)
        + [pltpu.SemaphoreType.DMA((4, owners // 2))],
        compiler_params=pltpu.CompilerParams(
            collective_id=4, has_side_effects=True, vmem_limit_bytes=60 * 1024 * 1024
        ),
        cost_estimate=lasting(45),
        name="ffn_in",
    )(shard, w_gate, w_up)


def ffn_back_kernel(
    chips,
    given,
    w_down,
    gate_in,
    up_in,
    rows_out,
    gate_out,
    up_out,
    rows,
    down_w,
    gate,
    upward,
    grad_gate,
    grad_up,
    own_sem,
    send_sem,
    land_sem,
    out_sem,
):
    own = lax.axis_index("fsdp")
    local = pltpu.make_async_copy(given, rows.at[own], own_sem.at[0])
    local.start()
    load = [
        pltpu.make_async_copy(w_down, down_w, own_sem.at[1]),
        pltpu.make_async_copy(gate_in, gate, own_sem.at[2]),
        pltpu.make_async_copy(up_in, upward, own_sem.at[3]),
    ]
    for copy in load:
        copy.start()
    greet_line(own, chips)

    def stores(other):
        place = pl.ds(other * 2, 2)
        pairs = ((rows, rows_out), (grad_gate, gate_out), (grad_up, up_out))
        return [
            pltpu.make_async_copy(source.at[place], target.at[place], out_sem.at[item, other])
            for item, (source, target) in enumerate(pairs)
        ]

    def use(other):
        left = chip_rows(rows, other)
        height = rows.shape[1]

        def tile(columns):
            grad_hidden = lax.dot_general(
                left, down_w[columns, :], (((1,), (1,)), ((), ())), preferred_element_type=f32
            )
            for half in range(2):
                grad = grad_hidden[half * height : (half + 1) * height]
                gated, raised = (
                    gate[other * 2 + half, :, columns],
                    upward[other * 2 + half, :, columns],
                )
                sigma = jax.nn.sigmoid(gated)
                grad_gate[other * 2 + half, :, columns] = (
                    grad * raised * sigma * (1.0 + gated * (1.0 - sigma))
                ).astype(bf16)
                grad_up[other * 2 + half, :, columns] = (grad * (gated * sigma)).astype(bf16)

        each_tile(down_w.shape[0], tile)
        for copy in stores(other):
            copy.start()

    def loaded():
        for copy in load:
            copy.wait()

    pass_along(chips, given, rows, local, send_sem, land_sem, loaded, use)
    for other in range(chips):
        for copy in stores(other):
            copy.wait()


def ffn_back(shard, w_down, gate, upward):
    owners = lax.axis_size("fsdp")
    rows, width = shard.shape
    units = w_down.shape[0]
    wide, narrow = (owners, rows, width), (owners, rows, units)
    return pl.pallas_call(
        functools.partial(ffn_back_kernel, owners // 2),
        out_shape=[
            jax.ShapeDtypeStruct(wide, bf16),
            jax.ShapeDtypeStruct(narrow, bf16),
            jax.ShapeDtypeStruct(narrow, bf16),
        ],
        in_specs=[in_vmem(), anywhere(), anywhere(), anywhere()],
        out_specs=[anywhere()] * 3,
        scratch_shapes=[
            pltpu.VMEM(wide, bf16),
            pltpu.VMEM((units, width), bf16),
            pltpu.VMEM(narrow, f32),
            pltpu.VMEM(narrow, f32),
            pltpu.VMEM(narrow, bf16),
            pltpu.VMEM(narrow, bf16),
            pltpu.SemaphoreType.DMA((4,)),
        ]
        + line_semaphores(owners)
        + [pltpu.SemaphoreType.DMA((3, owners // 2))],
        compiler_params=pltpu.CompilerParams(
            collective_id=5, has_side_effects=True, vmem_limit_bytes=60 * 1024 * 1024
        ),
        cost_estimate=lasting(45),
        name="ffn_back",
    )(shard, w_down, gate, upward)


def reduce_kernel(chips, wire, count, turned, *refs):
    left_in, right_in, total = refs[:count], refs[count : 2 * count], refs[2 * count]
    refs = refs[2 * count + 1 :]
    left, right, refs = refs[:count], refs[count : 2 * count], refs[2 * count :]
    mine, aside, beside, from_left, from_right, outgoing = refs[:6]
    load_sem, side_send, side_land, line_send, left_land, right_land = refs[6:]
    own = lax.axis_index("fsdp")
    chip, core = own // 2, own % 2
    sibling = chip * 2 + 1 - core
    rows = total.shape[0]

    def side(other):
        return remote(
            aside.at[other],
            beside.at[other],
            side_send.at[other],
            side_land.at[other],
            {"fsdp": sibling},
        )

    def rightward(other, target):
        return remote(
            outgoing.at[other],
            from_left.at[other],
            line_send.at[other],
            left_land.at[other],
            {"fsdp": target},
        )

    def leftward(other, target):
        return remote(
            outgoing.at[other],
            from_right.at[other],
            line_send.at[other],
            right_land.at[other],
            {"fsdp": target},
        )

    load = [
        pltpu.make_async_copy(source, target, load_sem.at[item])
        for item, (source, target) in enumerate(zip(left_in + right_in, left + right))
    ]
    for copy in load:
        copy.start()
    greet_line(own, chips)
    for copy in load:
        copy.wait()

    def multiply(other):
        lefts = [chip_rows(ref, other) for ref in left]

        def tile(columns):
            product = None
            for item in range(count):
                if turned:
                    part = lax.dot_general(
                        lefts[item],
                        right[item][columns, :],
                        (((1,), (1,)), ((), ())),
                        preferred_element_type=f32,
                    )
                else:
                    part = jnp.dot(
                        lefts[item], right[item][:, columns], preferred_element_type=f32
                    )
                product = part if product is None else product + part

            @pl.when(core == 0)
            def _():
                mine[other, :, columns] = product[:rows]
                aside[other, :, columns] = product[rows:]

            @pl.when(core == 1)
            def _():
                mine[other, :, columns] = product[rows:]
                aside[other, :, columns] = product[:rows]

        each_tile(total.shape[1], tile)
        side(other).start()

    def each_turn(right_does, left_does):
        for tick in range(chips - 1):
            right_to = chips - 1 - (tick - chip)
            left_to = tick - (chips - 1 - chip)

            @pl.when((tick >= chip) & (right_to > chip))
            def _():
                right_does(right_to)

            @pl.when((left_to >= 0) & (left_to < chip))
            def _():
                left_does(left_to)

    each_turn(multiply, multiply)
    multiply(chip)

    def send_right(other):
        side(other).wait_recv()

        @pl.when(chip > 0)
        def _():
            rightward(other, own).wait_recv()
            outgoing[other] = (
                mine[other] + beside[other] + from_left[other].astype(f32)
            ).astype(wire)

        @pl.when(chip == 0)
        def _():
            outgoing[other] = (mine[other] + beside[other]).astype(wire)

        rightward(other, own + 2).start()

    def send_left(other):
        side(other).wait_recv()

        @pl.when(chip < chips - 1)
        def _():
            leftward(other, own).wait_recv()
            outgoing[other] = (
                mine[other] + beside[other] + from_right[other].astype(f32)
            ).astype(wire)

        @pl.when(chip == chips - 1)
        def _():
            outgoing[other] = (mine[other] + beside[other]).astype(wire)

        leftward(other, own - 2).start()

    each_turn(send_right, send_left)
    side(chip).wait_recv()
    total[...] = mine[chip] + beside[chip]

    @pl.when(chip > 0)
    def _():
        rightward(chip, own).wait_recv()
        total[...] += from_left[chip].astype(f32)

    @pl.when(chip < chips - 1)
    def _():
        leftward(chip, own).wait_recv()
        total[...] += from_right[chip].astype(f32)

    for other in range(chips):
        side(other).wait_send()

        @pl.when(chip != other)
        def _():
            rightward(other, own).wait_send()


def reduce_line(lefts, rights, key, turned=False, wire=bf16):
    owners, rows, _ = lefts[0].shape
    width = rights[0].shape[0 if turned else 1]
    chips, count = owners // 2, len(lefts)
    return pl.pallas_call(
        functools.partial(reduce_kernel, chips, wire, count, turned),
        out_shape=jax.ShapeDtypeStruct((rows, width), f32),
        in_specs=[anywhere()] * (2 * count),
        out_specs=in_vmem(),
        scratch_shapes=[pltpu.VMEM(item.shape, item.dtype) for item in lefts + rights]
        + [
            pltpu.VMEM((chips, rows, width), f32),
            pltpu.VMEM((chips, rows, width), f32),
            pltpu.VMEM((chips, rows, width), f32),
            pltpu.VMEM((chips, rows, width), wire),
            pltpu.VMEM((chips, rows, width), wire),
            pltpu.VMEM((chips, rows, width), wire),
            pltpu.SemaphoreType.DMA((2 * count,)),
            pltpu.SemaphoreType.DMA((chips,)),
            pltpu.SemaphoreType.DMA((chips,)),
            pltpu.SemaphoreType.DMA((chips,)),
            pltpu.SemaphoreType.DMA((chips,)),
            pltpu.SemaphoreType.DMA((chips,)),
        ],
        compiler_params=pltpu.CompilerParams(
            collective_id=key, has_side_effects=True, vmem_limit_bytes=63 * 1024 * 1024
        ),
        cost_estimate=lasting(45),
        name=f"reduce_line_{key}",
    )(*lefts, *rights)


def greet_peers(axes):
    barrier = pltpu.get_barrier_semaphore()
    expected = 0
    for axis in axes:
        own, size = lax.axis_index(axis), lax.axis_size(axis)
        for step in range(1, size):
            pl.semaphore_signal(
                barrier, inc=1, device_id={axis: lax.rem(own + step, size)}, device_id_type=MESH
            )
        expected += size - 1
    pl.semaphore_wait(barrier, expected)


def start_kernel(
    owners,
    parts,
    tokens,
    small,
    inverse,
    w_query,
    w_key,
    w_value,
    group_tokens,
    small_all,
    heads_w,
    cosines,
    sines,
    own_sem,
    small_send,
    small_land,
    piece_send,
    piece_land,
    part_send,
    part_land,
    line_send,
    line_land,
):
    own, part = lax.axis_index("fsdp"), lax.axis_index("ctx")
    piece, own_width = heads_w.shape[2], heads_w.shape[3] // 3
    weights = (w_query, w_key, w_value)

    def cut(item, place):
        return weights[item].at[
            pl.ds(pl.multiple_of(part * piece, piece), piece),
            pl.ds(pl.multiple_of(place * own_width, own_width), own_width),
        ]

    def slot(item, place):
        return heads_w.at[place, part, :, pl.ds(item * own_width, own_width)]

    local_tokens = pltpu.make_async_copy(tokens, group_tokens.at[own], own_sem.at[0])
    local_small = pltpu.make_async_copy(small, small_all.at[own], own_sem.at[1])
    local_pieces = [
        pltpu.make_async_copy(cut(item, own), slot(item, own), own_sem.at[2 + item])
        for item in range(3)
    ]
    for copy in [local_tokens, local_small] + local_pieces:
        copy.start()
    greet_peers(("fsdp", "ctx"))
    first = []
    for step in range(1, owners):
        peer = lax.rem(own + step, owners)
        for item in range(3):
            first.append(
                remote(
                    cut(item, peer),
                    slot(item, own),
                    piece_send.at[item, step],
                    piece_land.at[item, step],
                    {"fsdp": peer},
                )
            )
        first.append(
            remote(
                small,
                small_all.at[own],
                small_send.at[step],
                small_land.at[step],
                {"fsdp": peer},
            )
        )
    for copy in first:
        copy.start()
    for copy in [local_small] + local_pieces:
        copy.wait()

    seq_rows = cosines.shape[0]
    angle = (
        lax.broadcasted_iota(jnp.int32, (seq_rows, HEAD_DIM), 0).astype(f32) * inverse[...]
    )
    cosines[...] = jnp.cos(angle)
    lane = lax.broadcasted_iota(jnp.int32, (seq_rows, HEAD_DIM), 1)
    sines[...] = jnp.sin(angle) * jnp.where(lane < HEAD_DIM // 2, -1.0, 1.0)

    def relay():
        for copy in first:
            copy.wait_recv()
        second = []
        for step in range(1, parts):
            second.append(
                remote(
                    heads_w.at[:, part],
                    heads_w.at[:, part],
                    part_send.at[step],
                    part_land.at[step],
                    {"ctx": lax.rem(part + step, parts)},
                )
            )
            second[-1].start()
        return second

    second = pass_along(
        owners // 2, tokens, group_tokens, local_tokens, line_send, line_land, relay
    )
    for copy in first:
        copy.wait_send()
    for copy in second:
        copy.wait()


def start(tokens, small, weights, parts, owners):
    rows, width = tokens.shape
    own_width = width // owners
    piece = weights[0].shape[0] // parts
    inverse = rope_base ** (-(np.arange(HEAD_DIM // 2, dtype=np.float32) * 2.0) / HEAD_DIM)
    inverse = jnp.asarray(np.concatenate([inverse, inverse])[None], f32)
    return pl.pallas_call(
        functools.partial(start_kernel, owners, parts),
        out_shape=[
            jax.ShapeDtypeStruct((owners, rows, width), bf16),
            jax.ShapeDtypeStruct((owners,) + small.shape, f32),
            jax.ShapeDtypeStruct((owners, parts, piece, 3 * own_width), bf16),
            jax.ShapeDtypeStruct((parts * rows, HEAD_DIM), f32),
            jax.ShapeDtypeStruct((parts * rows, HEAD_DIM), f32),
        ],
        in_specs=[in_vmem(), in_vmem(), in_vmem(), anywhere(), anywhere(), anywhere()],
        out_specs=[anywhere(), anywhere(), anywhere(), in_vmem(), in_vmem()],
        scratch_shapes=[
            pltpu.SemaphoreType.DMA((5,)),
            pltpu.SemaphoreType.DMA((owners,)),
            pltpu.SemaphoreType.DMA((owners,)),
            pltpu.SemaphoreType.DMA((3, owners)),
            pltpu.SemaphoreType.DMA((3, owners)),
            pltpu.SemaphoreType.DMA((parts,)),
            pltpu.SemaphoreType.DMA((parts,)),
        ]
        + line_semaphores(owners),
        compiler_params=pltpu.CompilerParams(collective_id=0, has_side_effects=True),
        cost_estimate=lasting(60),
        name="start",
    )(tokens, small, inverse, *weights)


def as_row(column):
    rows = column.shape[0]
    return jnp.broadcast_to(column, (rows, 128)).T[:1]


def as_column(row):
    rows = row.shape[1]
    return jnp.broadcast_to(row, (128, rows)).T[:, :1]


def share_stats(stats, everyone, send_sem, land_sem):
    own, owners = lax.axis_index("fsdp"), lax.axis_size("fsdp")
    copies = []
    for step in range(1, owners):
        copies.append(
            remote(
                stats,
                everyone.at[own],
                send_sem.at[step],
                land_sem.at[step],
                {"fsdp": lax.rem(own + step, owners)},
            )
        )
        copies[-1].start()
    everyone[own] = stats[...]
    for copy in copies:
        copy.wait()
    total = everyone[0]
    for place in range(1, owners):
        total += everyone[place]
    return total


def table_rows(table, row_block, rows, block_rows):
    def block(at):
        taken = table[at * block_rows : (at + 1) * block_rows]
        return jnp.concatenate([taken] * (rows // block_rows), axis=0)

    found = block(0)
    for at in range(1, table.shape[0] // block_rows):
        found = jnp.where(row_block == at, block(at), found)
    return found


def each_head(width):
    return [slice(at, at + HEAD_DIM) for at in range(0, width, HEAD_DIM)]


def heads_kernel(
    block_rows,
    row_blocks,
    tokens,
    weights,
    cosines,
    sines,
    gains,
    packed,
    raw,
    scales,
    stage,
    stats,
    everyone,
    own_sem,
    stat_send,
    stat_land,
    part_send,
    part_land,
):
    owners, rows, width = tokens.shape
    parts, own_width = stage.shape[0], stage.shape[-1]
    pair = owners // parts
    part = lax.axis_index("ctx")
    greet_peers(("fsdp", "ctx"))

    def project(seq, carry):
        product = jnp.dot(tokens[seq], weights[...], preferred_element_type=f32)
        for kind in range(2):
            values = product[:, kind * own_width : (kind + 1) * own_width]
            raw[kind, seq] = values
            stats[pl.ds(kind * owners + seq, 1), :] = as_row(
                jnp.sum(values * values, axis=-1, keepdims=True)
            )
        stage[seq // pair, 2, seq % pair] = product[:, 2 * own_width :].astype(bf16)
        return carry

    lax.fori_loop(0, owners, project, 0)
    scales[...] = lax.rsqrt(share_stats(stats, everyone, stat_send, stat_land) / width + norm_eps)

    def rotate(seq, carry):
        row_block = row_blocks[seq]
        cosine = table_rows(cosines, row_block, rows, block_rows)
        sine = table_rows(sines, row_block, rows, block_rows)
        for kind in range(2):
            scale = as_column(scales[pl.ds(kind * owners + seq, 1), :])
            for head in each_head(own_width):
                values = raw[kind, seq, :, head] * scale * gains[kind : kind + 1, head]
                stage[seq // pair, kind, seq % pair, :, head] = (
                    values * cosine + pltpu.roll(values, HEAD_DIM // 2, 1) * sine
                ).astype(bf16)
        return carry

    copies = []
    for step in range(1, parts + 1):
        peer = lax.rem(part + step, parts)
        lax.fori_loop(peer * pair, (peer + 1) * pair, rotate, 0)
        if step < parts:
            copies.append(
                remote(
                    stage.at[peer],
                    packed.at[part],
                    part_send.at[step],
                    part_land.at[step],
                    {"ctx": peer},
                )
            )
        else:
            copies.append(pltpu.make_async_copy(stage.at[part], packed.at[part], own_sem))
        copies[-1].start()
    for copy in copies:
        copy.wait()


def heads(row_blocks, tokens, weights, cosines, sines, gains, parts, block_rows):
    owners, rows, width = tokens.shape
    own_width = width // owners
    pair = owners // parts
    packed = (parts, 3, pair, rows, own_width)
    return pl.pallas_call(
        functools.partial(heads_kernel, block_rows),
        out_shape=[
            jax.ShapeDtypeStruct(packed, bf16),
            jax.ShapeDtypeStruct((2, owners, rows, own_width), f32),
            jax.ShapeDtypeStruct((2 * owners, rows), f32),
        ],
        in_specs=[in_vmem()] * 6,
        out_specs=[anywhere(), in_vmem(), in_vmem()],
        scratch_shapes=[
            pltpu.VMEM(packed, bf16),
            pltpu.VMEM((2 * owners, rows), f32),
            pltpu.VMEM((owners, 2 * owners, rows), f32),
            pltpu.SemaphoreType.DMA,
            pltpu.SemaphoreType.DMA((owners,)),
            pltpu.SemaphoreType.DMA((owners,)),
            pltpu.SemaphoreType.DMA((parts,)),
            pltpu.SemaphoreType.DMA((parts,)),
        ],
        compiler_params=pltpu.CompilerParams(
            collective_id=1, has_side_effects=True, vmem_limit_bytes=60 * 1024 * 1024
        ),
        cost_estimate=lasting(35),
        name="heads",
    )(row_blocks, tokens, weights, cosines, sines, gains)


def heads_back_kernel(
    block_rows,
    row_blocks,
    grad_query,
    grad_key,
    grad_value,
    cosines,
    sines,
    gains,
    raw,
    scales,
    grads,
    gain_sums,
    pair_grads,
    pair_values,
    stats,
    everyone,
    own_sem,
    stat_send,
    stat_land,
    part_send,
    part_land,
):
    kinds, owners, rows, own_width = raw.shape
    parts = pair_values.shape[0]
    pair = owners // parts
    width = owners * own_width
    part = lax.axis_index("ctx")
    sources = (grad_query, grad_key, grad_value)

    def landing(item, place):
        return pair_values.at[place] if item == 2 else pair_grads.at[item, place]

    local = [
        pltpu.make_async_copy(sources[item].at[part], landing(item, part), own_sem.at[item])
        for item in range(3)
    ]
    for copy in local:
        copy.start()
    greet_peers(("fsdp", "ctx"))
    copies = []
    for step in range(1, parts):
        peer = lax.rem(part + step, parts)
        for item in range(3):
            copies.append(
                remote(
                    sources[item].at[peer],
                    landing(item, part),
                    part_send.at[item, step],
                    part_land.at[item, step],
                    {"ctx": peer},
                )
            )
            copies[-1].start()
    gain_sums[...] = jnp.zeros_like(gain_sums)
    for copy in local:
        copy.wait()
    for copy in copies:
        copy.wait()

    def unrotate(seq, carry):
        row_block = row_blocks[seq]
        cosine = table_rows(cosines, row_block, rows, block_rows)
        sine = table_rows(sines, row_block, rows, block_rows)
        for kind in range(kinds):
            scale = as_column(scales[pl.ds(kind * owners + seq, 1), :])
            products = jnp.zeros((rows, 1), f32)
            for head in each_head(own_width):
                rotated = pair_grads[kind, seq // pair, seq % pair, :, head]
                values = rotated * cosine - pltpu.roll(rotated, HEAD_DIM // 2, 1) * sine
                plain = raw[kind, seq, :, head]
                gain_sums[kind : kind + 1, head] += jnp.sum(
                    values * (plain * scale), axis=0, keepdims=True
                )
                values = values * gains[kind : kind + 1, head]
                pair_grads[kind, seq // pair, seq % pair, :, head] = values
                products += jnp.sum(values * plain, axis=-1, keepdims=True)
            stats[pl.ds(kind * owners + seq, 1), :] = as_row(products)
        return carry

    lax.fori_loop(0, owners, unrotate, 0)
    means = share_stats(stats, everyone, stat_send, stat_land) / width
    stats[...] = means

    def through_norm(seq, carry):
        for kind in range(kinds):
            row = pl.ds(kind * owners + seq, 1)
            scale, mean = as_column(scales[row, :]), as_column(stats[row, :])
            grads[seq, :, kind * own_width : (kind + 1) * own_width] = (
                scale * pair_grads[kind, seq // pair, seq % pair]
                - raw[kind, seq] * (scale * scale * scale * mean)
            ).astype(bf16)
        grads[seq, :, 2 * own_width :] = pair_values[seq // pair, seq % pair]
        return carry

    lax.fori_loop(0, owners, through_norm, 0)


def heads_back(row_blocks, pair_grads, cosines, sines, gains, raw, scales, block_rows):
    kinds, owners, rows, own_width = raw.shape
    parts, pair = pair_grads[0].shape[:2]
    return pl.pallas_call(
        functools.partial(heads_back_kernel, block_rows),
        out_shape=[
            jax.ShapeDtypeStruct((owners, rows, 3 * own_width), bf16),
            jax.ShapeDtypeStruct((2, own_width), f32),
        ],
        in_specs=[in_vmem()] * 9,
        out_specs=[in_vmem(), in_vmem()],
        scratch_shapes=[
            pltpu.VMEM((2, parts, pair, rows, own_width), f32),
            pltpu.VMEM((parts, pair, rows, own_width), bf16),
            pltpu.VMEM((2 * owners, rows), f32),
            pltpu.VMEM((owners, 2 * owners, rows), f32),
            pltpu.SemaphoreType.DMA((3,)),
            pltpu.SemaphoreType.DMA((owners,)),
            pltpu.SemaphoreType.DMA((owners,)),
            pltpu.SemaphoreType.DMA((3, parts)),
            pltpu.SemaphoreType.DMA((3, parts)),
        ],
        compiler_params=pltpu.CompilerParams(
            collective_id=2, has_side_effects=True, vmem_limit_bytes=60 * 1024 * 1024
        ),
        cost_estimate=lasting(45),
        name="heads_back",
    )(row_blocks, *pair_grads, cosines, sines, gains, raw, scales)


def finish_kernel(
    owners,
    parts,
    sums,
    gain_post,
    gain_heads,
    kept,
    gain_own,
    post_all,
    gain_mine,
    part_all,
    own_sem,
    piece_send,
    piece_land,
    part_send,
    part_land,
    post_send,
    post_land,
    gain_send,
    gain_land,
):
    own, part = lax.axis_index("fsdp"), lax.axis_index("ctx")
    width = kept.shape[3]
    own_width = width // owners

    def cut(item, place):
        start = pl.multiple_of((place * 3 + item) * own_width, own_width)
        return sums.at[:, pl.ds(start, own_width)]

    def slot(item):
        return kept.at[
            part, item, :, pl.ds(pl.multiple_of(own * own_width, own_width), own_width)
        ]

    output_rows = sums.at[:, pl.ds(3 * width, width)]
    local = [
        pltpu.make_async_copy(cut(item, own), slot(item), own_sem.at[item]) for item in range(3)
    ]
    local.append(pltpu.make_async_copy(output_rows, kept.at[part, 3], own_sem.at[3]))
    for copy in local:
        copy.start()
    greet_peers(("fsdp", "ctx"))
    first, posts, second = [], [], []
    for step in range(1, owners):
        peer = lax.rem(own + step, owners)
        for item in range(3):
            first.append(
                remote(
                    cut(item, peer),
                    slot(item),
                    piece_send.at[item, step],
                    piece_land.at[item, step],
                    {"fsdp": peer},
                )
            )
        posts.append(
            remote(
                gain_post.at[peer],
                post_all.at[own],
                post_send.at[step],
                post_land.at[step],
                {"fsdp": peer},
            )
        )
    for copy in first + posts:
        copy.start()
    for step in range(1, parts):
        second.append(
            remote(
                output_rows,
                kept.at[part, 3],
                part_send.at[0, step],
                part_land.at[0, step],
                {"ctx": lax.rem(part + step, parts)},
            )
        )
        second[-1].start()
    post_all[own] = gain_post[own]
    for copy in local:
        copy.wait()
    for copy in first:
        copy.wait_recv()
    for step in range(1, parts):
        second.append(
            remote(
                kept.at[part, pl.ds(0, 3)],
                kept.at[part, pl.ds(0, 3)],
                part_send.at[1, step],
                part_land.at[1, step],
                {"ctx": lax.rem(part + step, parts)},
            )
        )
        second[-1].start()
    for copy in posts:
        copy.wait()
    post = post_all[0]
    for place in range(1, owners):
        post += post_all[place]
    gain_mine[:2, :] = gain_heads[...]
    gain_mine[2:, :] = post
    gains = []
    for step in range(1, parts):
        gains.append(
            remote(
                gain_mine,
                part_all.at[part],
                gain_send.at[step],
                gain_land.at[step],
                {"ctx": lax.rem(part + step, parts)},
            )
        )
        gains[-1].start()
    part_all[part] = gain_mine[...]
    for copy in gains:
        copy.wait()
    total = part_all[0]
    for place in range(1, parts):
        total += part_all[place]
    gain_own[...] = total
    for copy in first:
        copy.wait_send()
    for copy in second:
        copy.wait()


def finish(sums, gain_post, gain_heads):
    owners, parts = lax.axis_size("fsdp"), lax.axis_size("ctx")
    piece, columns = sums.shape
    width = columns // 4
    own_width = width // owners
    return pl.pallas_call(
        functools.partial(finish_kernel, owners, parts),
        out_shape=[
            jax.ShapeDtypeStruct((parts, 4, piece, width), bf16),
            jax.ShapeDtypeStruct((4, own_width), f32),
        ],
        in_specs=[in_vmem(), in_vmem(), in_vmem()],
        out_specs=[anywhere(), in_vmem()],
        scratch_shapes=[
            pltpu.VMEM((owners, 2, own_width), f32),
            pltpu.VMEM((4, own_width), f32),
            pltpu.VMEM((parts, 4, own_width), f32),
            pltpu.SemaphoreType.DMA((4,)),
            pltpu.SemaphoreType.DMA((3, owners)),
            pltpu.SemaphoreType.DMA((3, owners)),
            pltpu.SemaphoreType.DMA((2, parts)),
            pltpu.SemaphoreType.DMA((2, parts)),
            pltpu.SemaphoreType.DMA((owners,)),
            pltpu.SemaphoreType.DMA((owners,)),
            pltpu.SemaphoreType.DMA((parts,)),
            pltpu.SemaphoreType.DMA((parts,)),
        ],
        compiler_params=pltpu.CompilerParams(collective_id=3, has_side_effects=True),
        cost_estimate=lasting(50),
        name="finish",
    )(sums, gain_post, gain_heads)


def probs_of(query, key, query_pos, key_pos):
    scores = lax.dot_general(
        query, key, (((1,), (1,)), ((), ())), preferred_element_type=f32
    ) * (HEAD_DIM ** (-0.5))
    scores = jnp.where(key_pos <= query_pos, scores, neg_fill)
    expd = jnp.exp(scores - jnp.max(scores, axis=-1, keepdims=True))
    return expd / jnp.sum(expd, axis=-1, keepdims=True)


def flat(ref):
    return ref[...].reshape(ref.shape[0] * ref.shape[-2], ref.shape[-1])


def attend_kernel(query_ref, key_ref, value_ref, query_pos, key_pos, mixed_ref):
    probs = probs_of(flat(query_ref), flat(key_ref), query_pos[...], key_pos[...])
    mixed_ref[...] = jnp.dot(
        probs.astype(bf16), flat(value_ref), preferred_element_type=f32
    ).astype(bf16)


def attend_back_kernel(
    query_ref,
    key_ref,
    value_ref,
    query_pos,
    key_pos,
    grad_ref,
    grad_query_ref,
    grad_key_ref,
    grad_value_ref,
    key_sum,
    value_sum,
):
    step, steps = pl.program_id(2), pl.num_programs(2)
    score_scale = HEAD_DIM ** (-0.5)
    query, key, value = flat(query_ref), flat(key_ref), flat(value_ref)
    grad = grad_ref[...]
    probs = probs_of(query, key, query_pos[...], key_pos[...])
    grad_probs = lax.dot_general(
        grad, value, (((1,), (1,)), ((), ())), preferred_element_type=f32
    )
    grad_scores = (
        probs * (grad_probs - jnp.sum(probs * grad_probs, axis=-1, keepdims=True))
    ).astype(bf16)
    grad_query_ref[...] = jnp.dot(grad_scores, key, preferred_element_type=f32) * score_scale
    value_part = lax.dot_general(
        probs.astype(bf16), grad, (((0,), (0,)), ((), ())), preferred_element_type=f32
    )
    key_part = lax.dot_general(
        grad_scores, query, (((0,), (0,)), ((), ())), preferred_element_type=f32
    )

    @pl.when(step == 0)
    def _():
        key_sum[...] = key_part
        value_sum[...] = value_part

    @pl.when(step > 0)
    def _():
        key_sum[...] += key_part
        value_sum[...] += value_part

    @pl.when(step == steps - 1)
    def _():
        grad_key_ref[...] = (key_sum[...] * score_scale).reshape(grad_key_ref.shape)
        grad_value_ref[...] = value_sum[...].astype(bf16).reshape(grad_value_ref.shape)


def attention_specs(parts, rows, seq_rows):
    query = pl.BlockSpec((1, None, None, rows, HEAD_DIM), lambda i, h, c: (c, 0, i, 0, h))
    key = pl.BlockSpec((parts, None, None, rows, HEAD_DIM), lambda i, h, c: (0, 1, i, 0, h))
    value = pl.BlockSpec((parts, None, None, rows, HEAD_DIM), lambda i, h, c: (0, 2, i, 0, h))
    query_pos = pl.BlockSpec((None, None, rows, 1), lambda i, h, c: (i, c, 0, 0))
    key_pos = pl.BlockSpec((None, 1, seq_rows), lambda i, h, c: (i, 0, 0))
    row_block = pl.BlockSpec((None, None, rows, HEAD_DIM), lambda i, h, c: (c, i, 0, h))
    all_block = pl.BlockSpec((parts, None, rows, HEAD_DIM), lambda i, h, c: (0, i, 0, h))
    return [query, key, value, query_pos, key_pos], row_block, all_block


def attend(packed, query_pos, key_pos):
    parts, _, pair, rows, width = packed.shape
    seq_rows = parts * rows
    in_specs, row_block, _ = attention_specs(parts, rows, seq_rows)
    return pl.pallas_call(
        attend_kernel,
        grid=(pair, width // HEAD_DIM, parts),
        out_shape=jax.ShapeDtypeStruct((parts, pair, rows, width), bf16),
        in_specs=in_specs,
        out_specs=row_block,
        cost_estimate=lasting(12),
        name="attend",
    )(packed, packed, packed, query_pos, key_pos)


def attend_back(packed, query_pos, key_pos, grad):
    parts, _, pair, rows, width = packed.shape
    seq_rows = parts * rows
    in_specs, row_block, all_block = attention_specs(parts, rows, seq_rows)
    return pl.pallas_call(
        attend_back_kernel,
        grid=(pair, width // HEAD_DIM, parts),
        out_shape=[
            jax.ShapeDtypeStruct((parts, pair, rows, width), f32),
            jax.ShapeDtypeStruct((parts, pair, rows, width), f32),
            jax.ShapeDtypeStruct((parts, pair, rows, width), bf16),
        ],
        in_specs=in_specs + [row_block],
        out_specs=[row_block, all_block, all_block],
        scratch_shapes=[
            pltpu.VMEM((seq_rows, HEAD_DIM), f32),
            pltpu.VMEM((seq_rows, HEAD_DIM), f32),
        ],
        cost_estimate=lasting(16),
        name="attend_back",
    )(packed, packed, packed, query_pos, key_pos, grad)


def norm_stat(values):
    return lax.rsqrt(jnp.mean(values * values, axis=-1, keepdims=True) + norm_eps)


def norm_back(values, scale, gain, grad_out):
    weighted = grad_out * gain
    grad_values = scale * weighted - values * (scale * scale * scale) * jnp.mean(
        weighted * values, axis=-1, keepdims=True
    )
    grad_gain = jnp.sum(grad_out * (values * scale), axis=0)
    return (grad_values, grad_gain)


def mm(left, right):
    return jnp.dot(left, right, preferred_element_type=f32)


def mm_nt(left, right):
    return lax.dot_general(left, right, (((1,), (1,)), ((), ())), preferred_element_type=f32)


def mm_tn(left, right):
    return lax.dot_general(left, right, (((0,), (0,)), ((), ())), preferred_element_type=f32)


def shards(
    hidden_in,
    block_order,
    w_query,
    w_key,
    w_value,
    w_output,
    w_gate,
    w_up,
    w_down,
    norm_gains,
    out_grad,
):
    rows, width = hidden_in.shape[1:]
    parts, owners = lax.axis_size("ctx"), lax.axis_size("fsdp")
    part = lax.axis_index("ctx")
    group = owners * rows
    own_width = width // owners
    pair = owners // parts
    blocks = block_order.shape[1]
    block_rows = parts * rows // blocks
    tokens_b = hidden_in[0]
    tokens_f = tokens_b.astype(f32)
    own_gains = norm_gains.astype(f32)

    small = jnp.concatenate(
        [own_gains, jnp.pad(block_order.astype(f32), ((0, 0), (0, own_width - blocks)))], axis=0
    )
    group_tokens, small_all, w_heads, cosines, sines = start(
        tokens_b, small, (w_query, w_key, w_value), parts, owners
    )
    w_heads = w_heads.reshape(width, 3 * own_width)
    group_tokens, w_output_in = lax.optimization_barrier((group_tokens, w_output))
    full_output = lax.all_gather(w_output_in, "fsdp", axis=0, tiled=True)
    gains = small_all[:, :4].transpose(1, 0, 2).reshape(4, width)
    orders = small_all[:, 4, :blocks].astype(jnp.int32)

    own_blocks = rows // block_rows
    row_blocks = jnp.repeat(
        lax.dynamic_slice_in_dim(orders, part * own_blocks, own_blocks, 1), block_rows, axis=1
    )[:, :, None]
    packed, raw, scales = heads(
        row_blocks, group_tokens, w_heads, cosines, sines, own_gains[:2], parts, block_rows
    )
    offsets = jnp.arange(block_rows, dtype=jnp.int32)
    pair_orders = lax.dynamic_slice_in_dim(orders, part * pair, pair, 0)
    pair_pos = pair_orders[:, :, None] * block_rows + offsets[None, None, :]
    query_pos = pair_pos.reshape(pair, parts, rows, 1)
    key_pos = pair_pos.reshape(pair, 1, parts * rows)
    mixed_pair = attend(packed, query_pos, key_pos)
    (mixed_group,) = exchange("ctx", [mixed_pair], 6, takes=10)
    mixed_group = mixed_group.reshape(owners, rows, own_width)
    (mixed_own,) = exchange("fsdp", [mixed_group], 7, takes=14)
    mixed_own = mixed_own.transpose(1, 0, 2).reshape(rows, width)
    projected = mm(mixed_own, full_output)
    proj_scale = norm_stat(projected)
    residual = tokens_f + projected * proj_scale * gains[2]
    mlp_rows_in, gate, upward, hidden = ffn_in(residual.astype(bf16), w_gate, w_up)
    mlp_out = reduce_line([hidden], [w_down], 9)
    mlp_scale = norm_stat(mlp_out)
    block_out = residual + mlp_out * mlp_scale * gains[3]

    grad_y = out_grad[0].astype(f32)
    grad_mlp, gain_ff = norm_back(mlp_out, mlp_scale, gains[3], grad_y)
    grad_rows, grad_gate, grad_up = ffn_back(grad_mlp.astype(bf16), w_down, gate, upward)

    def summed_over_rows(left, right):
        left, right = left.reshape(group, -1), right.reshape(group, -1)
        return mm_tn(left, right).astype(bf16)

    grad_gate, grad_up, *ffn_parts = lax.optimization_barrier(
        (
            grad_gate,
            grad_up,
            summed_over_rows(mlp_rows_in, grad_gate),
            summed_over_rows(mlp_rows_in, grad_up),
            summed_over_rows(hidden, grad_rows),
        )
    )
    gate_sum, up_sum, down_sum = lax.psum(tuple(ffn_parts), "ctx")
    grad_res = grad_y + reduce_line([grad_gate, grad_up], [w_gate, w_up], 11, turned=True)
    grad_proj, gain_attn = norm_back(projected, proj_scale, gains[2], grad_res)
    grad_proj_rows = gather_line(grad_proj.astype(bf16), 12)
    grad_mixed = mm_nt(grad_proj_rows, w_output).astype(bf16)
    (grad_mixed,) = exchange(
        "ctx", [grad_mixed.reshape(parts, pair, rows, own_width)], 13, takes=10
    )
    pair_grads = attend_back(packed, query_pos, key_pos, grad_mixed)
    grad_heads, gain_heads = heads_back(
        row_blocks, pair_grads, cosines, sines, own_gains[:2], raw, scales, block_rows
    )

    piece = own_width // parts
    output_part = summed_over_rows(mixed_group, grad_proj_rows)
    heads_part = summed_over_rows(group_tokens, grad_heads)
    attention_part = jnp.concatenate(
        [
            heads_part.reshape(owners, parts, piece, 3 * own_width)
            .transpose(1, 2, 0, 3)
            .reshape(parts, piece, 3 * width),
            output_part.reshape(parts, piece, width),
        ],
        axis=2,
    )
    attention_part, down_sum, gate_sum, up_sum = lax.optimization_barrier(
        (attention_part, down_sum, gate_sum, up_sum)
    )
    attention_part = lax.psum_scatter(attention_part, "ctx", scatter_dimension=0, tiled=False)
    input_grad = grad_res + reduce_line([grad_heads], [w_heads], 16, turned=True)
    attention_part, input_grad = lax.optimization_barrier((attention_part, input_grad))
    gain_post = jnp.stack([gain_attn, gain_ff]).reshape(2, owners, own_width).transpose(1, 0, 2)
    attention_all, gain_own = finish(attention_part, gain_post, gain_heads)
    attention_all = [
        attention_all[:, item].reshape(own_width, width).astype(f32) for item in range(4)
    ]
    return (
        block_out.astype(bf16)[None],
        input_grad[None],
        *attention_all,
        gate_sum.astype(f32),
        up_sum.astype(f32),
        down_sum.astype(f32),
        gain_own,
    )


def solution(mesh):
    return jax.shard_map(
        shards,
        mesh=mesh,
        in_specs=(
            P("fsdp", "ctx", None),
            P("fsdp", None),
            P("fsdp", None),
            P("fsdp", None),
            P("fsdp", None),
            P("fsdp", None),
            P(None, "fsdp"),
            P(None, "fsdp"),
            P("fsdp", None),
            P(None, "fsdp"),
            P("fsdp", "ctx", None),
        ),
        out_specs=(
            P("fsdp", "ctx", None),
            P("fsdp", "ctx", None),
            P("fsdp", None),
            P("fsdp", None),
            P("fsdp", None),
            P("fsdp", None),
            P(None, "fsdp"),
            P(None, "fsdp"),
            P("fsdp", None),
            P(None, "fsdp"),
        ),
        check_vma=False,
    )
```

```python
import functools

import jax
import jax.numpy as jnp
import numpy as np
from jax import lax
from jax.experimental import pallas as pl
from jax.experimental.pallas import tpu as pltpu
from jax.sharding import PartitionSpec as P

HEADS = 16
HEAD_DIM = 128

norm_eps = 1e-06
rope_base = 500000.0
neg_fill = -1e30

MESH = pl.DeviceIdType.MESH
f32 = jnp.float32
bf16 = jnp.bfloat16


def anywhere():
    return pl.BlockSpec(memory_space=pl.ANY)


def in_vmem():
    return pl.BlockSpec(memory_space=pltpu.VMEM)


def lasting(microseconds):
    return pl.CostEstimate(
        flops=0, transcendentals=0, bytes_accessed=int(microseconds * 3_300_000)
    )


def remote(source, target, sent, landed, where):
    return pltpu.make_async_remote_copy(
        src_ref=source,
        dst_ref=target,
        send_sem=sent,
        recv_sem=landed,
        device_id=where,
        device_id_type=MESH,
    )


def exchange_kernel(axis, size, scatter, count, *refs):
    given, kept = refs[:count], refs[count : 2 * count]
    own_sem, send_sem, land_sem = refs[2 * count :]
    own = lax.axis_index(axis)
    barrier = pltpu.get_barrier_semaphore()
    for step in range(1, size):
        pl.semaphore_signal(
            barrier, inc=1, device_id={axis: lax.rem(own + step, size)}, device_id_type=MESH
        )
    local = []
    for item in range(count):
        source = given[item].at[own] if scatter else given[item]
        local.append(pltpu.make_async_copy(source, kept[item].at[own], own_sem.at[item]))
        local[-1].start()
    pl.semaphore_wait(barrier, size - 1)
    copies = []
    for step in range(1, size):
        peer = lax.rem(own + step, size)
        for item in range(count):
            source = given[item].at[peer] if scatter else given[item]
            copies.append(
                remote(
                    source,
                    kept[item].at[own],
                    send_sem.at[item, step],
                    land_sem.at[item, step],
                    {axis: peer},
                )
            )
            copies[-1].start()
    for copy in local:
        copy.wait()
    for copy in copies:
        copy.wait()


def exchange(axis, arrays, key, scatter=True, takes=6):
    size = lax.axis_size(axis)
    count = len(arrays)
    shapes = [
        jax.ShapeDtypeStruct(item.shape if scatter else (size,) + item.shape, item.dtype)
        for item in arrays
    ]
    return pl.pallas_call(
        functools.partial(exchange_kernel, axis, size, scatter, count),
        out_shape=shapes,
        in_specs=[in_vmem()] * count,
        out_specs=[anywhere()] * count,
        scratch_shapes=[
            pltpu.SemaphoreType.DMA((count,)),
            pltpu.SemaphoreType.DMA((count, size)),
            pltpu.SemaphoreType.DMA((count, size)),
        ],
        compiler_params=pltpu.CompilerParams(collective_id=key, has_side_effects=True),
        cost_estimate=lasting(takes),
        name=f"exchange_{axis}_{key}",
    )(*arrays)


def greet_line(own, chips):
    chip, core = own // 2, own % 2
    barrier = pltpu.get_barrier_semaphore()

    def greet(place):
        pl.semaphore_signal(barrier, inc=1, device_id={"fsdp": place}, device_id_type=MESH)

    greet(chip * 2 + 1 - core)

    @pl.when(chip > 0)
    def _():
        greet(own - 2)

    @pl.when(chip < chips - 1)
    def _():
        greet(own + 2)

    expected = 1 + jnp.minimum(chip, 1) + jnp.minimum(chips - 1 - chip, 1)
    pl.semaphore_wait(barrier, expected)


CUTS = 4


def pass_along(chips, given, kept, local, send_sem, land_sem, between=None, use=None):
    own = lax.axis_index("fsdp")
    chip, core = own // 2, own % 2
    sibling = chip * 2 + 1 - core
    height = given.shape[0] // CUTS

    def copy(source, place, way, step, cut, target):
        rows = pl.ds(cut * height, height)
        return remote(
            source.at[rows],
            kept.at[place, rows],
            send_sem.at[way, step, cut],
            land_sem.at[place, cut],
            {"fsdp": target},
        )

    def both_ways(step, cut, left_does, right_does):
        from_left, from_right = own - 2 * step, own + 2 * step

        @pl.when(chip >= step)
        def _():
            left_does(from_left, step, cut)

        @pl.when(chip + step < chips)
        def _():
            right_does(from_right, step, cut)

    def hand_on(way, nearer, side):
        def does(place, step, cut):
            copy(kept.at[place], place, way, step, cut, own).wait_recv()

            @pl.when((chip < chips - 1) if way == 0 else (chip > 0))
            def _():
                copy(kept.at[place], place, way, step, cut, nearer).start()

            copy(kept.at[place], place, side, step, cut, sibling).start()

        return does

    def sent(way, nearer, side):
        def does(place, step, cut):
            @pl.when((chip < chips - 1) if way == 0 else (chip > 0))
            def _():
                copy(kept.at[place], place, way, step, cut, nearer).wait_send()

            copy(kept.at[place], place, side, step, cut, sibling).wait_send()

        return does

    def from_sibling(other):
        place = other * 2 + 1 - core
        for cut in range(CUTS):
            copy(kept.at[place], place, 2, 0, cut, sibling).wait_recv()
        if use:
            use(other)

    for cut in range(CUTS):

        @pl.when(chip < chips - 1)
        def _():
            copy(given, own, 0, 0, cut, own + 2).start()

        @pl.when(chip > 0)
        def _():
            copy(given, own, 1, 0, cut, own - 2).start()

        copy(given, own, 2, 0, cut, sibling).start()
    local.wait()
    result = between() if between else None
    from_sibling(chip)
    for step in range(1, chips):
        for cut in range(CUTS):
            both_ways(step, cut, hand_on(0, own + 2, 2), hand_on(1, own - 2, 3))

        @pl.when(chip >= step)
        def _():
            from_sibling(chip - step)

        @pl.when(chip + step < chips)
        def _():
            from_sibling(chip + step)

    for cut in range(CUTS):

        @pl.when(chip < chips - 1)
        def _():
            copy(given, own, 0, 0, cut, own + 2).wait_send()

        @pl.when(chip > 0)
        def _():
            copy(given, own, 1, 0, cut, own - 2).wait_send()

        copy(given, own, 2, 0, cut, sibling).wait_send()
        for step in range(1, chips):
            both_ways(step, cut, sent(0, own + 2, 2), sent(1, own - 2, 3))
    return result


def line_semaphores(owners):
    return [
        pltpu.SemaphoreType.DMA((4, owners // 2, CUTS)),
        pltpu.SemaphoreType.DMA((owners, CUTS)),
    ]


def gather_kernel(chips, given, kept, own_sem, send_sem, land_sem):
    own = lax.axis_index("fsdp")
    local = pltpu.make_async_copy(given, kept.at[own], own_sem)
    local.start()
    greet_line(own, chips)
    pass_along(chips, given, kept, local, send_sem, land_sem)


def gather_line(shard, key):
    size = lax.axis_size("fsdp")
    kept = pl.pallas_call(
        functools.partial(gather_kernel, size // 2),
        out_shape=jax.ShapeDtypeStruct((size,) + shard.shape, shard.dtype),
        in_specs=[in_vmem()],
        out_specs=anywhere(),
        scratch_shapes=[pltpu.SemaphoreType.DMA] + line_semaphores(size),
        compiler_params=pltpu.CompilerParams(collective_id=key, has_side_effects=True),
        cost_estimate=lasting(40),
        name=f"gather_line_{key}",
    )(shard)
    return kept.reshape((size * shard.shape[0],) + shard.shape[1:])


TILE = 512


def each_tile(columns, does):
    width = min(TILE, columns)

    def step(at, carry):
        does(pl.ds(pl.multiple_of(at * width, width), width))
        return carry

    lax.fori_loop(0, columns // width, step, 0)


def chip_rows(ref, other):
    taken = ref[pl.ds(other * 2, 2)]
    return taken.reshape(2 * taken.shape[1], taken.shape[2])


def put_chip(ref, other, columns, values):
    rows = ref.shape[1]
    ref[other * 2, :, columns] = values[:rows]
    ref[other * 2 + 1, :, columns] = values[rows:]


def ffn_in_kernel(
    chips,
    given,
    w_gate,
    w_up,
    rows_out,
    gate_out,
    up_out,
    hidden_out,
    rows,
    gate_w,
    up_w,
    gate,
    upward,
    hidden,
    own_sem,
    send_sem,
    land_sem,
    out_sem,
):
    own = lax.axis_index("fsdp")
    local = pltpu.make_async_copy(given, rows.at[own], own_sem.at[0])
    local.start()
    load = [
        pltpu.make_async_copy(w_gate, gate_w, own_sem.at[1]),
        pltpu.make_async_copy(w_up, up_w, own_sem.at[2]),
    ]
    for copy in load:
        copy.start()
    greet_line(own, chips)

    def stores(other):
        place = pl.ds(other * 2, 2)
        pairs = ((rows, rows_out), (gate, gate_out), (upward, up_out), (hidden, hidden_out))
        return [
            pltpu.make_async_copy(source.at[place], target.at[place], out_sem.at[item, other])
            for item, (source, target) in enumerate(pairs)
        ]

    def use(other):
        left = chip_rows(rows, other)

        def tile(columns):
            gated = jnp.dot(left, gate_w[:, columns], preferred_element_type=f32)
            raised = jnp.dot(left, up_w[:, columns], preferred_element_type=f32)
            put_chip(gate, other, columns, gated)
            put_chip(upward, other, columns, raised)
            put_chip(
                hidden, other, columns, (gated * jax.nn.sigmoid(gated) * raised).astype(bf16)
            )

        each_tile(gate_w.shape[1], tile)
        for copy in stores(other):
            copy.start()

    def loaded():
        for copy in load:
            copy.wait()

    pass_along(chips, given, rows, local, send_sem, land_sem, loaded, use)
    for other in range(chips):
        for copy in stores(other):
            copy.wait()


def ffn_in(shard, w_gate, w_up):
    owners = lax.axis_size("fsdp")
    rows, width = shard.shape
    units = w_gate.shape[1]
    wide, narrow = (owners, rows, width), (owners, rows, units)
    return pl.pallas_call(
        functools.partial(ffn_in_kernel, owners // 2),
        out_shape=[
            jax.ShapeDtypeStruct(wide, bf16),
            jax.ShapeDtypeStruct(narrow, f32),
            jax.ShapeDtypeStruct(narrow, f32),
            jax.ShapeDtypeStruct(narrow, bf16),
        ],
        in_specs=[in_vmem(), anywhere(), anywhere()],
        out_specs=[anywhere()] * 4,
        scratch_shapes=[
            pltpu.VMEM(wide, bf16),
            pltpu.VMEM((width, units), bf16),
            pltpu.VMEM((width, units), bf16),
            pltpu.VMEM(narrow, f32),
            pltpu.VMEM(narrow, f32),
            pltpu.VMEM(narrow, bf16),
            pltpu.SemaphoreType.DMA((3,)),
        ]
        + line_semaphores(owners)
        + [pltpu.SemaphoreType.DMA((4, owners // 2))],
        compiler_params=pltpu.CompilerParams(
            collective_id=4, has_side_effects=True, vmem_limit_bytes=60 * 1024 * 1024
        ),
        cost_estimate=lasting(45),
        name="ffn_in",
    )(shard, w_gate, w_up)


def ffn_back_kernel(
    chips,
    given,
    w_down,
    gate_in,
    up_in,
    rows_out,
    gate_out,
    up_out,
    rows,
    down_w,
    gate,
    upward,
    grad_gate,
    grad_up,
    own_sem,
    send_sem,
    land_sem,
    out_sem,
):
    own = lax.axis_index("fsdp")
    local = pltpu.make_async_copy(given, rows.at[own], own_sem.at[0])
    local.start()
    load = [
        pltpu.make_async_copy(w_down, down_w, own_sem.at[1]),
        pltpu.make_async_copy(gate_in, gate, own_sem.at[2]),
        pltpu.make_async_copy(up_in, upward, own_sem.at[3]),
    ]
    for copy in load:
        copy.start()
    greet_line(own, chips)

    def stores(other):
        place = pl.ds(other * 2, 2)
        pairs = ((rows, rows_out), (grad_gate, gate_out), (grad_up, up_out))
        return [
            pltpu.make_async_copy(source.at[place], target.at[place], out_sem.at[item, other])
            for item, (source, target) in enumerate(pairs)
        ]

    def use(other):
        left = chip_rows(rows, other)
        height = rows.shape[1]

        def tile(columns):
            grad_hidden = lax.dot_general(
                left, down_w[columns, :], (((1,), (1,)), ((), ())), preferred_element_type=f32
            )
            for half in range(2):
                grad = grad_hidden[half * height : (half + 1) * height]
                gated, raised = (
                    gate[other * 2 + half, :, columns],
                    upward[other * 2 + half, :, columns],
                )
                sigma = jax.nn.sigmoid(gated)
                grad_gate[other * 2 + half, :, columns] = (
                    grad * raised * sigma * (1.0 + gated * (1.0 - sigma))
                ).astype(bf16)
                grad_up[other * 2 + half, :, columns] = (grad * (gated * sigma)).astype(bf16)

        each_tile(down_w.shape[0], tile)
        for copy in stores(other):
            copy.start()

    def loaded():
        for copy in load:
            copy.wait()

    pass_along(chips, given, rows, local, send_sem, land_sem, loaded, use)
    for other in range(chips):
        for copy in stores(other):
            copy.wait()


def ffn_back(shard, w_down, gate, upward):
    owners = lax.axis_size("fsdp")
    rows, width = shard.shape
    units = w_down.shape[0]
    wide, narrow = (owners, rows, width), (owners, rows, units)
    return pl.pallas_call(
        functools.partial(ffn_back_kernel, owners // 2),
        out_shape=[
            jax.ShapeDtypeStruct(wide, bf16),
            jax.ShapeDtypeStruct(narrow, bf16),
            jax.ShapeDtypeStruct(narrow, bf16),
        ],
        in_specs=[in_vmem(), anywhere(), anywhere(), anywhere()],
        out_specs=[anywhere()] * 3,
        scratch_shapes=[
            pltpu.VMEM(wide, bf16),
            pltpu.VMEM((units, width), bf16),
            pltpu.VMEM(narrow, f32),
            pltpu.VMEM(narrow, f32),
            pltpu.VMEM(narrow, bf16),
            pltpu.VMEM(narrow, bf16),
            pltpu.SemaphoreType.DMA((4,)),
        ]
        + line_semaphores(owners)
        + [pltpu.SemaphoreType.DMA((3, owners // 2))],
        compiler_params=pltpu.CompilerParams(
            collective_id=5, has_side_effects=True, vmem_limit_bytes=60 * 1024 * 1024
        ),
        cost_estimate=lasting(45),
        name="ffn_back",
    )(shard, w_down, gate, upward)


HALVES = 2
STRIP = 16


def reduce_kernel(chips, wire, count, turned, *refs):
    left_in, right_in, total = refs[:count], refs[count : 2 * count], refs[2 * count]
    refs = refs[2 * count + 1 :]
    left, right, refs = refs[:count], refs[count : 2 * count], refs[2 * count :]
    products, beside, from_left, from_right, outgoing = refs[:5]
    load_sem, side_send, side_land, line_send, left_land, right_land = refs[5:]
    own = lax.axis_index("fsdp")
    chip, core = own // 2, own % 2
    sibling = chip * 2 + 1 - core
    height = total.shape[0] // HALVES
    last = chips - 1

    def side(other, half):
        rows = pl.ds(half * height, height)
        return remote(
            products.at[other * 2 + 1 - core, rows],
            beside.at[other, rows],
            side_send.at[other, half],
            side_land.at[other, half],
            {"fsdp": sibling},
        )

    def rightward(other, half, target):
        rows = pl.ds(half * height, height)
        return remote(
            outgoing.at[other, rows],
            from_left.at[other, rows],
            line_send.at[other, half],
            left_land.at[other, half],
            {"fsdp": target},
        )

    def leftward(other, half, target):
        rows = pl.ds(half * height, height)
        return remote(
            outgoing.at[other, rows],
            from_right.at[other, rows],
            line_send.at[other, half],
            right_land.at[other, half],
            {"fsdp": target},
        )

    load = [
        pltpu.make_async_copy(source, target, load_sem.at[item])
        for item, (source, target) in enumerate(zip(left_in + right_in, left + right))
    ]
    for copy in load:
        copy.start()
    greet_line(own, chips)
    for copy in load:
        copy.wait()

    def multiply(other):
        lefts = [chip_rows(ref, other) for ref in left]

        def tile(columns):
            product = None
            for item in range(count):
                if turned:
                    part = lax.dot_general(
                        lefts[item],
                        right[item][columns, :],
                        (((1,), (1,)), ((), ())),
                        preferred_element_type=f32,
                    )
                else:
                    part = jnp.dot(
                        lefts[item], right[item][:, columns], preferred_element_type=f32
                    )
                product = part if product is None else product + part
            put_chip(products, other, columns, product)

        each_tile(total.shape[1], tile)
        for half in range(HALVES):
            side(other, half).start()

    def add_up(other, half, inbound, target):
        def strip(at, carry):
            rows = pl.ds(pl.multiple_of(half * height + at * STRIP, STRIP), STRIP)
            value = products[other * 2 + core, rows] + beside[other, rows]
            for ref in inbound:
                value += ref[other, rows].astype(f32)
            if target is total:
                total[rows] = value
            else:
                target[other, rows] = value.astype(wire)
            return carry

        lax.fori_loop(0, height // STRIP, strip, 0)

    def send_right(other, inbound):
        for half in range(HALVES):
            side(other, half).wait_recv()
            if inbound:
                rightward(other, half, own).wait_recv()
            add_up(other, half, inbound, outgoing)
            rightward(other, half, own + 2).start()

    def send_left(other, inbound):
        for half in range(HALVES):
            side(other, half).wait_recv()
            if inbound:
                leftward(other, half, own).wait_recv()
            add_up(other, half, inbound, outgoing)
            leftward(other, half, own - 2).start()

    def each_turn(does):
        def turn(at, carry):
            tick, leftwards = at // 2, at % 2
            right_to, left_to = last - (tick - chip), tick - (last - chip)
            goes_right = (leftwards == 0) & (tick >= chip) & (right_to > chip)
            goes_left = (leftwards == 1) & (left_to >= 0) & (left_to < chip)
            does(jnp.where(leftwards == 0, right_to, left_to), goes_right, goes_left, tick)
            return carry

        lax.fori_loop(0, 2 * last, turn, 0)

    def multiply_turn(other, goes_right, goes_left, tick):
        @pl.when(goes_right | goes_left)
        def _():
            multiply(other)

        @pl.when(goes_right & (chip == 0) & (tick > 0))
        def _():
            send_right(other + 1, ())

        @pl.when(goes_left & (chip == last) & (tick > 0))
        def _():
            send_left(other - 1, ())

    def send_turn(other, goes_right, goes_left, tick):
        @pl.when(goes_right & (chip > 0))
        def _():
            send_right(other, (from_left,))

        @pl.when(goes_left & (chip < last))
        def _():
            send_left(other, (from_right,))

    each_turn(multiply_turn)
    multiply(chip)

    @pl.when(chip == 0)
    def _():
        send_right(1, ())

    @pl.when(chip == last)
    def _():
        send_left(last - 1, ())

    each_turn(send_turn)
    for half in range(HALVES):
        side(chip, half).wait_recv()

        @pl.when(chip > 0)
        def _():
            rightward(chip, half, own).wait_recv()

        @pl.when(chip < last)
        def _():
            leftward(chip, half, own).wait_recv()

        @pl.when(chip == 0)
        def _():
            add_up(chip, half, (from_right,), total)

        @pl.when(chip == last)
        def _():
            add_up(chip, half, (from_left,), total)

        @pl.when((chip > 0) & (chip < last))
        def _():
            add_up(chip, half, (from_left, from_right), total)

    for other in range(chips):
        for half in range(HALVES):
            side(other, half).wait_send()

            @pl.when(chip != other)
            def _():
                rightward(other, half, own).wait_send()


def reduce_line(lefts, rights, key, turned=False, wire=bf16):
    owners, rows, _ = lefts[0].shape
    width = rights[0].shape[0 if turned else 1]
    chips, count = owners // 2, len(lefts)
    return pl.pallas_call(
        functools.partial(reduce_kernel, chips, wire, count, turned),
        out_shape=jax.ShapeDtypeStruct((rows, width), f32),
        in_specs=[anywhere()] * (2 * count),
        out_specs=in_vmem(),
        scratch_shapes=[pltpu.VMEM(item.shape, item.dtype) for item in lefts + rights]
        + [
            pltpu.VMEM((owners, rows, width), f32),
            pltpu.VMEM((chips, rows, width), f32),
            pltpu.VMEM((chips, rows, width), wire),
            pltpu.VMEM((chips, rows, width), wire),
            pltpu.VMEM((chips, rows, width), wire),
            pltpu.SemaphoreType.DMA((2 * count,)),
        ]
        + [pltpu.SemaphoreType.DMA((chips, HALVES))] * 5,
        compiler_params=pltpu.CompilerParams(
            collective_id=key, has_side_effects=True, vmem_limit_bytes=63 * 1024 * 1024
        ),
        cost_estimate=lasting(45),
        name=f"reduce_line_{key}",
    )(*lefts, *rights)


def greet_peers(axes):
    barrier = pltpu.get_barrier_semaphore()
    expected = 0
    for axis in axes:
        own, size = lax.axis_index(axis), lax.axis_size(axis)
        for step in range(1, size):
            pl.semaphore_signal(
                barrier, inc=1, device_id={axis: lax.rem(own + step, size)}, device_id_type=MESH
            )
        expected += size - 1
    pl.semaphore_wait(barrier, expected)


def start_kernel(
    owners,
    parts,
    tokens,
    small,
    inverse,
    w_query,
    w_key,
    w_value,
    group_tokens,
    small_all,
    heads_w,
    cosines,
    sines,
    own_sem,
    small_send,
    small_land,
    piece_send,
    piece_land,
    part_send,
    part_land,
    line_send,
    line_land,
):
    own, part = lax.axis_index("fsdp"), lax.axis_index("ctx")
    piece, own_width = heads_w.shape[2], heads_w.shape[3] // 3
    weights = (w_query, w_key, w_value)

    def cut(item, place):
        return weights[item].at[
            pl.ds(pl.multiple_of(part * piece, piece), piece),
            pl.ds(pl.multiple_of(place * own_width, own_width), own_width),
        ]

    def slot(item, place):
        return heads_w.at[place, part, :, pl.ds(item * own_width, own_width)]

    local_tokens = pltpu.make_async_copy(tokens, group_tokens.at[own], own_sem.at[0])
    local_small = pltpu.make_async_copy(small, small_all.at[own], own_sem.at[1])
    local_pieces = [
        pltpu.make_async_copy(cut(item, own), slot(item, own), own_sem.at[2 + item])
        for item in range(3)
    ]
    for copy in [local_tokens, local_small] + local_pieces:
        copy.start()
    greet_peers(("fsdp", "ctx"))
    first = []
    for step in range(1, owners):
        peer = lax.rem(own + step, owners)
        for item in range(3):
            first.append(
                remote(
                    cut(item, peer),
                    slot(item, own),
                    piece_send.at[item, step],
                    piece_land.at[item, step],
                    {"fsdp": peer},
                )
            )
        first.append(
            remote(
                small,
                small_all.at[own],
                small_send.at[step],
                small_land.at[step],
                {"fsdp": peer},
            )
        )
    for copy in first:
        copy.start()
    for copy in [local_small] + local_pieces:
        copy.wait()

    seq_rows = cosines.shape[0]
    angle = (
        lax.broadcasted_iota(jnp.int32, (seq_rows, HEAD_DIM), 0).astype(f32) * inverse[...]
    )
    cosines[...] = jnp.cos(angle)
    lane = lax.broadcasted_iota(jnp.int32, (seq_rows, HEAD_DIM), 1)
    sines[...] = jnp.sin(angle) * jnp.where(lane < HEAD_DIM // 2, -1.0, 1.0)

    def relay():
        for copy in first:
            copy.wait_recv()
        second = []
        for step in range(1, parts):
            second.append(
                remote(
                    heads_w.at[:, part],
                    heads_w.at[:, part],
                    part_send.at[step],
                    part_land.at[step],
                    {"ctx": lax.rem(part + step, parts)},
                )
            )
            second[-1].start()
        return second

    second = pass_along(
        owners // 2, tokens, group_tokens, local_tokens, line_send, line_land, relay
    )
    for copy in first:
        copy.wait_send()
    for copy in second:
        copy.wait()


def start(tokens, small, weights, parts, owners):
    rows, width = tokens.shape
    own_width = width // owners
    piece = weights[0].shape[0] // parts
    inverse = rope_base ** (-(np.arange(HEAD_DIM // 2, dtype=np.float32) * 2.0) / HEAD_DIM)
    inverse = jnp.asarray(np.concatenate([inverse, inverse])[None], f32)
    return pl.pallas_call(
        functools.partial(start_kernel, owners, parts),
        out_shape=[
            jax.ShapeDtypeStruct((owners, rows, width), bf16),
            jax.ShapeDtypeStruct((owners,) + small.shape, f32),
            jax.ShapeDtypeStruct((owners, parts, piece, 3 * own_width), bf16),
            jax.ShapeDtypeStruct((parts * rows, HEAD_DIM), f32),
            jax.ShapeDtypeStruct((parts * rows, HEAD_DIM), f32),
        ],
        in_specs=[in_vmem(), in_vmem(), in_vmem(), anywhere(), anywhere(), anywhere()],
        out_specs=[anywhere(), anywhere(), anywhere(), in_vmem(), in_vmem()],
        scratch_shapes=[
            pltpu.SemaphoreType.DMA((5,)),
            pltpu.SemaphoreType.DMA((owners,)),
            pltpu.SemaphoreType.DMA((owners,)),
            pltpu.SemaphoreType.DMA((3, owners)),
            pltpu.SemaphoreType.DMA((3, owners)),
            pltpu.SemaphoreType.DMA((parts,)),
            pltpu.SemaphoreType.DMA((parts,)),
        ]
        + line_semaphores(owners),
        compiler_params=pltpu.CompilerParams(collective_id=0, has_side_effects=True),
        cost_estimate=lasting(60),
        name="start",
    )(tokens, small, inverse, *weights)


def as_row(column):
    rows = column.shape[0]
    return jnp.broadcast_to(column, (rows, 128)).T[:1]


def as_column(row):
    rows = row.shape[1]
    return jnp.broadcast_to(row, (128, rows)).T[:, :1]


def share_stats(stats, everyone, send_sem, land_sem):
    own, owners = lax.axis_index("fsdp"), lax.axis_size("fsdp")
    copies = []
    for step in range(1, owners):
        copies.append(
            remote(
                stats,
                everyone.at[own],
                send_sem.at[step],
                land_sem.at[step],
                {"fsdp": lax.rem(own + step, owners)},
            )
        )
        copies[-1].start()
    everyone[own] = stats[...]
    for copy in copies:
        copy.wait()
    total = everyone[0]
    for place in range(1, owners):
        total += everyone[place]
    return total


def table_rows(table, row_block, rows, block_rows):
    def block(at):
        taken = table[at * block_rows : (at + 1) * block_rows]
        return jnp.concatenate([taken] * (rows // block_rows), axis=0)

    found = block(0)
    for at in range(1, table.shape[0] // block_rows):
        found = jnp.where(row_block == at, block(at), found)
    return found


def each_head(width):
    return [slice(at, at + HEAD_DIM) for at in range(0, width, HEAD_DIM)]


def heads_kernel(
    block_rows,
    row_blocks,
    tokens,
    weights,
    cosines,
    sines,
    gains,
    packed,
    raw,
    scales,
    stage,
    stats,
    everyone,
    own_sem,
    stat_send,
    stat_land,
    part_send,
    part_land,
):
    owners, rows, width = tokens.shape
    parts, own_width = stage.shape[0], stage.shape[-1]
    pair = owners // parts
    part = lax.axis_index("ctx")
    greet_peers(("fsdp", "ctx"))

    def project(seq, carry):
        product = jnp.dot(tokens[seq], weights[...], preferred_element_type=f32)
        for kind in range(2):
            values = product[:, kind * own_width : (kind + 1) * own_width]
            raw[kind, seq] = values
            stats[pl.ds(kind * owners + seq, 1), :] = as_row(
                jnp.sum(values * values, axis=-1, keepdims=True)
            )
        stage[seq // pair, 2, seq % pair] = product[:, 2 * own_width :].astype(bf16)
        return carry

    lax.fori_loop(0, owners, project, 0)
    scales[...] = lax.rsqrt(share_stats(stats, everyone, stat_send, stat_land) / width + norm_eps)

    def rotate(seq, carry):
        row_block = row_blocks[seq]
        cosine = table_rows(cosines, row_block, rows, block_rows)
        sine = table_rows(sines, row_block, rows, block_rows)
        for kind in range(2):
            scale = as_column(scales[pl.ds(kind * owners + seq, 1), :])
            for head in each_head(own_width):
                values = raw[kind, seq, :, head] * scale * gains[kind : kind + 1, head]
                stage[seq // pair, kind, seq % pair, :, head] = (
                    values * cosine + pltpu.roll(values, HEAD_DIM // 2, 1) * sine
                ).astype(bf16)
        return carry

    copies = []
    for step in range(1, parts + 1):
        peer = lax.rem(part + step, parts)
        lax.fori_loop(peer * pair, (peer + 1) * pair, rotate, 0)
        if step < parts:
            copies.append(
                remote(
                    stage.at[peer],
                    packed.at[part],
                    part_send.at[step],
                    part_land.at[step],
                    {"ctx": peer},
                )
            )
        else:
            copies.append(pltpu.make_async_copy(stage.at[part], packed.at[part], own_sem))
        copies[-1].start()
    for copy in copies:
        copy.wait()


def heads(row_blocks, tokens, weights, cosines, sines, gains, parts, block_rows):
    owners, rows, width = tokens.shape
    own_width = width // owners
    pair = owners // parts
    packed = (parts, 3, pair, rows, own_width)
    return pl.pallas_call(
        functools.partial(heads_kernel, block_rows),
        out_shape=[
            jax.ShapeDtypeStruct(packed, bf16),
            jax.ShapeDtypeStruct((2, owners, rows, own_width), f32),
            jax.ShapeDtypeStruct((2 * owners, rows), f32),
        ],
        in_specs=[in_vmem()] * 6,
        out_specs=[anywhere(), in_vmem(), in_vmem()],
        scratch_shapes=[
            pltpu.VMEM(packed, bf16),
            pltpu.VMEM((2 * owners, rows), f32),
            pltpu.VMEM((owners, 2 * owners, rows), f32),
            pltpu.SemaphoreType.DMA,
            pltpu.SemaphoreType.DMA((owners,)),
            pltpu.SemaphoreType.DMA((owners,)),
            pltpu.SemaphoreType.DMA((parts,)),
            pltpu.SemaphoreType.DMA((parts,)),
        ],
        compiler_params=pltpu.CompilerParams(
            collective_id=1, has_side_effects=True, vmem_limit_bytes=60 * 1024 * 1024
        ),
        cost_estimate=lasting(35),
        name="heads",
    )(row_blocks, tokens, weights, cosines, sines, gains)


def heads_back_kernel(
    block_rows,
    row_blocks,
    grad_query,
    grad_key,
    grad_value,
    cosines,
    sines,
    gains,
    raw,
    scales,
    grads,
    gain_sums,
    landed,
    weighted,
    stats,
    everyone,
    own_sem,
    stat_send,
    stat_land,
    part_send,
    part_land,
):
    kinds, owners, rows, own_width = raw.shape
    parts = landed.shape[1]
    pair = owners // parts
    width = owners * own_width
    part = lax.axis_index("ctx")
    sources = (grad_query, grad_key, grad_value)

    def landing(item, place):
        return landed.at[item, place]

    local = [
        pltpu.make_async_copy(sources[item].at[part], landing(item, part), own_sem.at[item])
        for item in range(3)
    ]
    for copy in local:
        copy.start()
    greet_peers(("fsdp", "ctx"))
    copies = []
    for step in range(1, parts):
        peer = lax.rem(part + step, parts)
        for item in range(3):
            copies.append(
                remote(
                    sources[item].at[peer],
                    landing(item, part),
                    part_send.at[item, step],
                    part_land.at[item, step],
                    {"ctx": peer},
                )
            )
            copies[-1].start()
    gain_sums[...] = jnp.zeros_like(gain_sums)
    for copy in local:
        copy.wait()
    for copy in copies:
        copy.wait()

    def unrotate(seq, carry):
        row_block = row_blocks[seq]
        cosine = table_rows(cosines, row_block, rows, block_rows)
        sine = table_rows(sines, row_block, rows, block_rows)
        for kind in range(kinds):
            scale = as_column(scales[pl.ds(kind * owners + seq, 1), :])
            products = jnp.zeros((rows, 1), f32)
            for head in each_head(own_width):
                rotated = landed[kind, seq // pair, seq % pair, :, head].astype(f32)
                values = rotated * cosine - pltpu.roll(rotated, HEAD_DIM // 2, 1) * sine
                plain = raw[kind, seq, :, head]
                gain_sums[kind : kind + 1, head] += jnp.sum(
                    values * (plain * scale), axis=0, keepdims=True
                )
                values = values * gains[kind : kind + 1, head]
                weighted[kind, seq, :, head] = values
                products += jnp.sum(values * plain, axis=-1, keepdims=True)
            stats[pl.ds(kind * owners + seq, 1), :] = as_row(products)
        return carry

    lax.fori_loop(0, owners, unrotate, 0)
    means = share_stats(stats, everyone, stat_send, stat_land) / width
    stats[...] = means

    def through_norm(seq, carry):
        for kind in range(kinds):
            row = pl.ds(kind * owners + seq, 1)
            scale, mean = as_column(scales[row, :]), as_column(stats[row, :])
            grads[seq, :, kind * own_width : (kind + 1) * own_width] = (
                scale * weighted[kind, seq]
                - raw[kind, seq] * (scale * scale * scale * mean)
            ).astype(bf16)
        grads[seq, :, 2 * own_width :] = landed[2, seq // pair, seq % pair]
        return carry

    lax.fori_loop(0, owners, through_norm, 0)


def heads_back(row_blocks, pair_grads, cosines, sines, gains, raw, scales, block_rows):
    kinds, owners, rows, own_width = raw.shape
    parts, pair = pair_grads[0].shape[:2]
    return pl.pallas_call(
        functools.partial(heads_back_kernel, block_rows),
        out_shape=[
            jax.ShapeDtypeStruct((owners, rows, 3 * own_width), bf16),
            jax.ShapeDtypeStruct((2, own_width), f32),
        ],
        in_specs=[in_vmem()] * 9,
        out_specs=[in_vmem(), in_vmem()],
        scratch_shapes=[
            pltpu.VMEM((3, parts, pair, rows, own_width), bf16),
            pltpu.VMEM((2, owners, rows, own_width), f32),
            pltpu.VMEM((2 * owners, rows), f32),
            pltpu.VMEM((owners, 2 * owners, rows), f32),
            pltpu.SemaphoreType.DMA((3,)),
            pltpu.SemaphoreType.DMA((owners,)),
            pltpu.SemaphoreType.DMA((owners,)),
            pltpu.SemaphoreType.DMA((3, parts)),
            pltpu.SemaphoreType.DMA((3, parts)),
        ],
        compiler_params=pltpu.CompilerParams(
            collective_id=2, has_side_effects=True, vmem_limit_bytes=60 * 1024 * 1024
        ),
        cost_estimate=lasting(45),
        name="heads_back",
    )(row_blocks, *pair_grads, cosines, sines, gains, raw, scales)


def finish_kernel(
    owners,
    parts,
    sums,
    gain_post,
    gain_heads,
    kept,
    kept_output,
    gain_own,
    post_all,
    gain_mine,
    part_all,
    own_sem,
    piece_send,
    piece_land,
    part_send,
    part_land,
    post_send,
    post_land,
    gain_send,
    gain_land,
):
    own, part = lax.axis_index("fsdp"), lax.axis_index("ctx")
    width = kept.shape[3]
    own_width = width // owners

    def cut(item, place):
        start = pl.multiple_of((place * 3 + item) * own_width, own_width)
        return sums.at[:, pl.ds(start, own_width)]

    def slot(item):
        return kept.at[
            part, item, :, pl.ds(pl.multiple_of(own * own_width, own_width), own_width)
        ]

    output_rows = sums.at[:, pl.ds(3 * width, width)]
    local = [
        pltpu.make_async_copy(cut(item, own), slot(item), own_sem.at[item]) for item in range(3)
    ]
    local.append(pltpu.make_async_copy(output_rows, kept_output.at[part], own_sem.at[3]))
    for copy in local:
        copy.start()
    greet_peers(("fsdp", "ctx"))
    first, posts, second = [], [], []
    for step in range(1, owners):
        peer = lax.rem(own + step, owners)
        first.append(
            [
                remote(
                    cut(item, peer),
                    slot(item),
                    piece_send.at[item, step],
                    piece_land.at[item, step],
                    {"fsdp": peer},
                )
                for item in range(3)
            ]
        )
        posts.append(
            remote(
                gain_post.at[peer],
                post_all.at[own],
                post_send.at[step],
                post_land.at[step],
                {"fsdp": peer},
            )
        )
    for copy in sum(first, []) + posts:
        copy.start()

    def spread(region, turn):
        for step in range(1, parts):
            second.append(
                remote(
                    region,
                    region,
                    part_send.at[turn, step],
                    part_land.at[turn, step],
                    {"ctx": lax.rem(part + step, parts)},
                )
            )
            second[-1].start()

    local[3].wait()
    spread(kept_output.at[part], owners)
    post_all[own] = gain_post[own]
    for copy in local[:3]:
        copy.wait()
    for turn in range(owners):
        if turn:
            for copy in first[turn - 1]:
                copy.wait_recv()
        place = lax.rem(own - turn + owners, owners)
        spread(
            kept.at[
                part, :, :, pl.ds(pl.multiple_of(place * own_width, own_width), own_width)
            ],
            turn,
        )
    for copy in posts:
        copy.wait()
    post = post_all[0]
    for place in range(1, owners):
        post += post_all[place]
    gain_mine[:2, :] = gain_heads[...]
    gain_mine[2:, :] = post
    gains = []
    for step in range(1, parts):
        gains.append(
            remote(
                gain_mine,
                part_all.at[part],
                gain_send.at[step],
                gain_land.at[step],
                {"ctx": lax.rem(part + step, parts)},
            )
        )
        gains[-1].start()
    part_all[part] = gain_mine[...]
    for copy in gains:
        copy.wait()
    total = part_all[0]
    for place in range(1, parts):
        total += part_all[place]
    gain_own[...] = total
    for copy in sum(first, []):
        copy.wait_send()
    for copy in second:
        copy.wait()


def finish(sums, gain_post, gain_heads):
    owners, parts = lax.axis_size("fsdp"), lax.axis_size("ctx")
    piece, columns = sums.shape
    width = columns // 4
    own_width = width // owners
    return pl.pallas_call(
        functools.partial(finish_kernel, owners, parts),
        out_shape=[
            jax.ShapeDtypeStruct((parts, 3, piece, width), bf16),
            jax.ShapeDtypeStruct((parts, piece, width), bf16),
            jax.ShapeDtypeStruct((4, own_width), f32),
        ],
        in_specs=[in_vmem(), in_vmem(), in_vmem()],
        out_specs=[anywhere(), anywhere(), in_vmem()],
        scratch_shapes=[
            pltpu.VMEM((owners, 2, own_width), f32),
            pltpu.VMEM((4, own_width), f32),
            pltpu.VMEM((parts, 4, own_width), f32),
            pltpu.SemaphoreType.DMA((4,)),
            pltpu.SemaphoreType.DMA((3, owners)),
            pltpu.SemaphoreType.DMA((3, owners)),
            pltpu.SemaphoreType.DMA((owners + 1, parts)),
            pltpu.SemaphoreType.DMA((owners + 1, parts)),
            pltpu.SemaphoreType.DMA((owners,)),
            pltpu.SemaphoreType.DMA((owners,)),
            pltpu.SemaphoreType.DMA((parts,)),
            pltpu.SemaphoreType.DMA((parts,)),
        ],
        compiler_params=pltpu.CompilerParams(collective_id=3, has_side_effects=True),
        cost_estimate=lasting(50),
        name="finish",
    )(sums, gain_post, gain_heads)


def widen_kernel(heads_ref, output_ref, *outs):
    for item in range(3):
        outs[item][...] = heads_ref[item].astype(f32)
    outs[3][...] = output_ref[...].astype(f32)


def widen(heads_sum, output_sum):
    parts, kinds, piece, width = heads_sum.shape
    return pl.pallas_call(
        widen_kernel,
        grid=(parts,),
        out_shape=[jax.ShapeDtypeStruct((parts * piece, width), f32)] * 4,
        in_specs=[
            pl.BlockSpec((None, kinds, piece, width), lambda c: (c, 0, 0, 0)),
            pl.BlockSpec((None, piece, width), lambda c: (c, 0, 0)),
        ],
        out_specs=[pl.BlockSpec((piece, width), lambda c: (c, 0))] * 4,
        cost_estimate=lasting(4),
        name="widen",
    )(heads_sum, output_sum)


def probs_of(query, key, query_pos, key_pos):
    scores = lax.dot_general(
        query, key, (((1,), (1,)), ((), ())), preferred_element_type=f32
    ) * (HEAD_DIM ** (-0.5))
    scores = jnp.where(key_pos <= query_pos, scores, neg_fill)
    expd = jnp.exp(scores - jnp.max(scores, axis=-1, keepdims=True))
    return expd / jnp.sum(expd, axis=-1, keepdims=True)


def flat(ref):
    return ref[...].reshape(ref.shape[0] * ref.shape[-2], ref.shape[-1])


def attend_kernel(query_ref, key_ref, value_ref, query_pos, key_pos, mixed_ref):
    probs = probs_of(flat(query_ref), flat(key_ref), query_pos[...], key_pos[...])
    mixed_ref[...] = jnp.dot(
        probs.astype(bf16), flat(value_ref), preferred_element_type=f32
    ).astype(bf16)


def attend_back_kernel(
    query_ref,
    key_ref,
    value_ref,
    query_pos,
    key_pos,
    grad_ref,
    grad_query_ref,
    grad_key_ref,
    grad_value_ref,
    key_sum,
    value_sum,
):
    step, steps = pl.program_id(2), pl.num_programs(2)
    score_scale = HEAD_DIM ** (-0.5)
    query, key, value = flat(query_ref), flat(key_ref), flat(value_ref)
    grad = grad_ref[...]
    probs = probs_of(query, key, query_pos[...], key_pos[...])
    grad_probs = lax.dot_general(
        grad, value, (((1,), (1,)), ((), ())), preferred_element_type=f32
    )
    grad_scores = (
        probs * (grad_probs - jnp.sum(probs * grad_probs, axis=-1, keepdims=True))
    ).astype(bf16)
    grad_query_ref[...] = (
        jnp.dot(grad_scores, key, preferred_element_type=f32) * score_scale
    ).astype(bf16)
    value_part = lax.dot_general(
        probs.astype(bf16), grad, (((0,), (0,)), ((), ())), preferred_element_type=f32
    )
    key_part = lax.dot_general(
        grad_scores, query, (((0,), (0,)), ((), ())), preferred_element_type=f32
    )

    @pl.when(step == 0)
    def _():
        key_sum[...] = key_part
        value_sum[...] = value_part

    @pl.when(step > 0)
    def _():
        key_sum[...] += key_part
        value_sum[...] += value_part

    @pl.when(step == steps - 1)
    def _():
        grad_key_ref[...] = (key_sum[...] * score_scale).astype(bf16).reshape(grad_key_ref.shape)
        grad_value_ref[...] = value_sum[...].astype(bf16).reshape(grad_value_ref.shape)


def attention_specs(parts, rows, seq_rows):
    query = pl.BlockSpec((1, None, None, rows, HEAD_DIM), lambda i, h, c: (c, 0, i, 0, h))
    key = pl.BlockSpec((parts, None, None, rows, HEAD_DIM), lambda i, h, c: (0, 1, i, 0, h))
    value = pl.BlockSpec((parts, None, None, rows, HEAD_DIM), lambda i, h, c: (0, 2, i, 0, h))
    query_pos = pl.BlockSpec((None, None, rows, 1), lambda i, h, c: (i, c, 0, 0))
    key_pos = pl.BlockSpec((None, 1, seq_rows), lambda i, h, c: (i, 0, 0))
    row_block = pl.BlockSpec((None, None, rows, HEAD_DIM), lambda i, h, c: (c, i, 0, h))
    all_block = pl.BlockSpec((parts, None, rows, HEAD_DIM), lambda i, h, c: (0, i, 0, h))
    return [query, key, value, query_pos, key_pos], row_block, all_block


def attend(packed, query_pos, key_pos):
    parts, _, pair, rows, width = packed.shape
    seq_rows = parts * rows
    in_specs, row_block, _ = attention_specs(parts, rows, seq_rows)
    return pl.pallas_call(
        attend_kernel,
        grid=(pair, width // HEAD_DIM, parts),
        out_shape=jax.ShapeDtypeStruct((parts, pair, rows, width), bf16),
        in_specs=in_specs,
        out_specs=row_block,
        cost_estimate=lasting(12),
        name="attend",
    )(packed, packed, packed, query_pos, key_pos)


def attend_back(packed, query_pos, key_pos, grad):
    parts, _, pair, rows, width = packed.shape
    seq_rows = parts * rows
    in_specs, row_block, all_block = attention_specs(parts, rows, seq_rows)
    return pl.pallas_call(
        attend_back_kernel,
        grid=(pair, width // HEAD_DIM, parts),
        out_shape=[jax.ShapeDtypeStruct((parts, pair, rows, width), bf16)] * 3,
        in_specs=in_specs + [row_block],
        out_specs=[row_block, all_block, all_block],
        scratch_shapes=[
            pltpu.VMEM((seq_rows, HEAD_DIM), f32),
            pltpu.VMEM((seq_rows, HEAD_DIM), f32),
        ],
        cost_estimate=lasting(16),
        name="attend_back",
    )(packed, packed, packed, query_pos, key_pos, grad)


def norm_stat(values):
    return lax.rsqrt(jnp.mean(values * values, axis=-1, keepdims=True) + norm_eps)


def norm_back(values, scale, gain, grad_out):
    weighted = grad_out * gain
    grad_values = scale * weighted - values * (scale * scale * scale) * jnp.mean(
        weighted * values, axis=-1, keepdims=True
    )
    grad_gain = jnp.sum(grad_out * (values * scale), axis=0)
    return (grad_values, grad_gain)


def mm(left, right):
    return jnp.dot(left, right, preferred_element_type=f32)


def mm_nt(left, right):
    return lax.dot_general(left, right, (((1,), (1,)), ((), ())), preferred_element_type=f32)


def mm_tn(left, right):
    return lax.dot_general(left, right, (((0,), (0,)), ((), ())), preferred_element_type=f32)


def shards(
    hidden_in,
    block_order,
    w_query,
    w_key,
    w_value,
    w_output,
    w_gate,
    w_up,
    w_down,
    norm_gains,
    out_grad,
):
    rows, width = hidden_in.shape[1:]
    parts, owners = lax.axis_size("ctx"), lax.axis_size("fsdp")
    part = lax.axis_index("ctx")
    group = owners * rows
    own_width = width // owners
    pair = owners // parts
    blocks = block_order.shape[1]
    block_rows = parts * rows // blocks
    tokens_b = hidden_in[0]
    tokens_f = tokens_b.astype(f32)
    own_gains = norm_gains.astype(f32)

    small = jnp.concatenate(
        [own_gains, jnp.pad(block_order.astype(f32), ((0, 0), (0, own_width - blocks)))], axis=0
    )
    group_tokens, small_all, w_heads, cosines, sines = start(
        tokens_b, small, (w_query, w_key, w_value), parts, owners
    )
    w_heads = w_heads.reshape(width, 3 * own_width)
    group_tokens, w_output_in = lax.optimization_barrier((group_tokens, w_output))
    full_output = lax.all_gather(w_output_in, "fsdp", axis=0, tiled=True)
    gains = small_all[:, :4].transpose(1, 0, 2).reshape(4, width)
    orders = small_all[:, 4, :blocks].astype(jnp.int32)

    own_blocks = rows // block_rows
    row_blocks = jnp.repeat(
        lax.dynamic_slice_in_dim(orders, part * own_blocks, own_blocks, 1), block_rows, axis=1
    )[:, :, None]
    packed, raw, scales = heads(
        row_blocks, group_tokens, w_heads, cosines, sines, own_gains[:2], parts, block_rows
    )
    offsets = jnp.arange(block_rows, dtype=jnp.int32)
    pair_orders = lax.dynamic_slice_in_dim(orders, part * pair, pair, 0)
    pair_pos = pair_orders[:, :, None] * block_rows + offsets[None, None, :]
    query_pos = pair_pos.reshape(pair, parts, rows, 1)
    key_pos = pair_pos.reshape(pair, 1, parts * rows)
    mixed_pair = attend(packed, query_pos, key_pos)
    (mixed_group,) = exchange("ctx", [mixed_pair], 6, takes=10)
    mixed_group = mixed_group.reshape(owners, rows, own_width)
    (mixed_own,) = exchange("fsdp", [mixed_group], 7, takes=14)
    mixed_own = mixed_own.transpose(1, 0, 2).reshape(rows, width)
    projected = mm(mixed_own, full_output)
    proj_scale = norm_stat(projected)
    residual = tokens_f + projected * proj_scale * gains[2]
    mlp_rows_in, gate, upward, hidden = ffn_in(residual.astype(bf16), w_gate, w_up)
    mlp_out = reduce_line([hidden], [w_down], 9)
    mlp_scale = norm_stat(mlp_out)
    block_out = residual + mlp_out * mlp_scale * gains[3]

    grad_y = out_grad[0].astype(f32)
    grad_mlp, gain_ff = norm_back(mlp_out, mlp_scale, gains[3], grad_y)
    grad_rows, grad_gate, grad_up = ffn_back(grad_mlp.astype(bf16), w_down, gate, upward)

    def summed_over_rows(left, right):
        left, right = left.reshape(group, -1), right.reshape(group, -1)
        return mm_tn(left, right).astype(bf16)

    grad_gate, grad_up, *ffn_parts = lax.optimization_barrier(
        (
            grad_gate,
            grad_up,
            summed_over_rows(mlp_rows_in, grad_gate),
            summed_over_rows(mlp_rows_in, grad_up),
            summed_over_rows(hidden, grad_rows),
        )
    )
    gate_sum, up_sum, down_sum = lax.psum(tuple(ffn_parts), "ctx")
    grad_res = grad_y + reduce_line([grad_gate, grad_up], [w_gate, w_up], 11, turned=True)
    grad_proj, gain_attn = norm_back(projected, proj_scale, gains[2], grad_res)
    grad_proj_rows = gather_line(grad_proj.astype(bf16), 12)
    grad_mixed = mm_nt(grad_proj_rows, w_output).astype(bf16)
    (grad_mixed,) = exchange(
        "ctx", [grad_mixed.reshape(parts, pair, rows, own_width)], 13, takes=10
    )
    pair_grads = attend_back(packed, query_pos, key_pos, grad_mixed)
    grad_heads, gain_heads = heads_back(
        row_blocks, pair_grads, cosines, sines, own_gains[:2], raw, scales, block_rows
    )

    piece = own_width // parts
    output_part = summed_over_rows(mixed_group, grad_proj_rows)
    heads_part = summed_over_rows(group_tokens, grad_heads)
    attention_part = jnp.concatenate(
        [
            heads_part.reshape(owners, parts, piece, 3 * own_width)
            .transpose(1, 2, 0, 3)
            .reshape(parts, piece, 3 * width),
            output_part.reshape(parts, piece, width),
        ],
        axis=2,
    )
    input_grad = grad_res + reduce_line([grad_heads], [w_heads], 16, turned=True)
    attention_part, input_grad, down_sum, gate_sum, up_sum = lax.optimization_barrier(
        (attention_part, input_grad, down_sum, gate_sum, up_sum)
    )
    attention_part = lax.psum_scatter(attention_part, "ctx", scatter_dimension=0, tiled=False)
    gain_post = jnp.stack([gain_attn, gain_ff]).reshape(2, owners, own_width).transpose(1, 0, 2)
    ffn_sums = [item.astype(f32) for item in (gate_sum, up_sum, down_sum)]
    attention_part, *ffn_sums = lax.optimization_barrier((attention_part, *ffn_sums))
    heads_sum, output_sum, gain_own = finish(attention_part, gain_post, gain_heads)
    return (
        block_out.astype(bf16)[None],
        input_grad[None],
        *widen(heads_sum, output_sum),
        *ffn_sums,
        gain_own,
    )


def solution(mesh):
    return jax.shard_map(
        shards,
        mesh=mesh,
        in_specs=(
            P("fsdp", "ctx", None),
            P("fsdp", None),
            P("fsdp", None),
            P("fsdp", None),
            P("fsdp", None),
            P("fsdp", None),
            P(None, "fsdp"),
            P(None, "fsdp"),
            P("fsdp", None),
            P(None, "fsdp"),
            P("fsdp", "ctx", None),
        ),
        out_specs=(
            P("fsdp", "ctx", None),
            P("fsdp", "ctx", None),
            P("fsdp", None),
            P("fsdp", None),
            P("fsdp", None),
            P("fsdp", None),
            P(None, "fsdp"),
            P(None, "fsdp"),
            P("fsdp", None),
            P(None, "fsdp"),
        ),
        check_vma=False,
    )
```
